256 devices in a mesh: group: 8 (over z), mp: 32 (over y, x, core).
Axes of the slice: x: 4, y: 4, z: 8, core: 2. Of those that a mesh axis runs over, the one named last changes fastest.
Arguments:
- option_latent_states: bfloat16 [2048, 8192], P('group', 'mp'), may hold values from -6 to 6
- mixer_scaling_factor: bfloat16 [1, 8192], P(None, 'mp'), may hold values from 0.099609375 to 1.8984375
- question_mapping_matrix: bfloat16 [8192, 8192], P(None, 'mp'), may hold values from -0.0625 to 0.0625
- lookup_content_matrix: bfloat16 [8192, 2048], P(None, 'mp'), may hold values from -0.0625 to 0.0625
- final_mapping_matrix: bfloat16 [8192, 8192], P('mp'), may hold values from -0.125 to 0.125
- payoff_readout_vector: bfloat16 [8192], P('mp'), may hold values from -0.0625 to 0.0625
- shared_trie_memo: bfloat16 [2, 512, 128, 1024], P(None, ('group', 'mp')), may hold values from -100 to 100
- option_route_pages: int32 [128, 32], P('group'), may hold values from 0 to 63, as said below
- option_page_tally: int32 [128], P('group'), may hold values from 1 to 32, as said below
- option_token_span: int32 [128], P('group'), may hold values from 1 to 16
- retained_pages: int32 [512], P(('group', 'mp')), may hold values from 0 to 1
- growth_place_mapping: int32 [768], P(('group', 'mp')), may hold values from 0 to 15, as said below
Outputs:
- scored_rows: bfloat16 [2048, 8192], P('group', 'mp')
- rewards: float32 [128], P('group')
- expanded: bfloat16 [2, 768, 128, 1024], P(None, ('group', 'mp'))
The draws below stay inside these ranges and needn't reach their ends.
Inputs may be any that keep to these rules, and one draw needn't show every extreme that they name: `option_route_pages`: the t-th listed block of a candidate is one of t * 2 to (t + 1) * 2 - 1; entries at or past option_page_tally are not read. `option_page_tally`: among the 16 candidates of each group index one lists all 32 blocks. `growth_place_mapping`: for every mp index, every survivor of every group index fills some slot.
All inputs are finite; a program needn't handle non-finite values.
Results may differ from the reference program's by a relative error of at most 0.005.
The reference program's roundings to bfloat16 on the way count: a program that leaves them out, or rounds other values in their place, can miss the bound.
Values may be sent and summed in bfloat16 or wider, within the bound.
No kernel may reach another device: no remote copies, remote signals or barrier semaphores. Data moves between devices by JAX's collectives and lax.ppermute only.
A program may use at most 128 MiB of HBM per device.

```python
import jax
import jax.numpy as jnp
from jax import lax

D = 8192
HEADS = 64
KVH = 8
HD = 128
BLK = 128
STEP = 16
RETAINED_NUMBER = 2
GROWTH_PLACES = 3
CAND_PAIR = 2
LOCAL_STORE_LOAD = 2
TBL = 32
CAND_G = 16
CANDS = 128
ROWS = 2048
POOL = 512
N_GROUP = 8
N_MP = 32


def draw_shared_trie_memo(key, part):
    cache_shape = (POOL, BLK, KVH * HD)
    key_one, key_two = jax.random.split(key, 2)
    stored_keys = 1.5 * jnp.clip(jax.random.normal(key_one, cache_shape, jnp.float32), -4.0, 4.0)
    stored_values = 3.0 * jnp.clip(jax.random.normal(key_two, cache_shape, jnp.float32), -4.0, 4.0)
    return jnp.stack([stored_keys, stored_values]).astype(jnp.bfloat16)


def draw_option_route_pages(key, part):
    offsets = jax.random.randint(key, (CANDS, TBL), 0, LOCAL_STORE_LOAD)
    return (jnp.arange(TBL, dtype=jnp.int32)[None, :] * LOCAL_STORE_LOAD + offsets).astype(jnp.int32)


def draw_option_page_tally(key, part):
    key_one, key_two = jax.random.split(jax.random.fold_in(key, 7))
    counts = jax.random.randint(key_one, (CANDS,), 1, TBL + 1)
    fullest = jax.random.randint(key_two, (N_GROUP,), 0, CAND_G)
    within = jnp.arange(CANDS, dtype=jnp.int32) % CAND_G
    owner_group = jnp.arange(CANDS, dtype=jnp.int32) // CAND_G
    return jnp.where(within == fullest[owner_group], TBL, counts).astype(jnp.int32)


def draw_growth_place_mapping(key, part):
    slot_count = N_GROUP * GROWTH_PLACES
    scores = jax.random.randint(jax.random.fold_in(key, 11), (N_MP, slot_count), 0, 1 << 20) * slot_count + jnp.arange(slot_count, dtype=jnp.int32)[None, :]
    sorted_order = jnp.argsort(scores, axis=1).astype(jnp.int32)
    chosen_labels = (sorted_order % (N_GROUP * RETAINED_NUMBER)).reshape(N_MP, N_GROUP, GROWTH_PLACES)
    return jnp.transpose(chosen_labels, (1, 0, 2)).reshape(-1).astype(jnp.int32)


def touch_ends(drawn, stream_key, least, top_value):
    place = [jax.random.randint(jax.random.fold_in(stream_key, axis), (), 0, length) for axis, length in enumerate(drawn.shape)]
    widest = drawn.shape.index(max(drawn.shape))
    neighbour = place[:widest] + [(place[widest] + 1) % drawn.shape[widest]] + place[widest + 1:]
    return drawn.at[tuple(place)].set(least).at[tuple(neighbour)].set(top_value)


def strengthened(drawn, own_key, source, target, blocks, factor):
    owner, partner = [(jnp.arange(drawn.shape[axis_at]) // (drawn.shape[axis_at] // blocks)).reshape([-1 if axis == axis_at else 1 for axis in range(drawn.ndim)]) for axis_at in (source, target)]
    chosen = jax.random.permutation(own_key, blocks)[partner]
    strong = (owner == chosen) | (owner == (partner + blocks // 2) % blocks)
    return jnp.where(strong, factor * drawn, drawn)


def shard_levels(stream_key, dims, shards, smallest, high):
    factor_of = 1.0
    for dim, parts in shards:
        draws = jax.random.uniform(jax.random.fold_in(jax.random.fold_in(stream_key, 6), dim), (parts,), jnp.float32, smallest / len(shards), high / len(shards))
        factor_of = factor_of * jnp.repeat(jnp.exp(draws), dims[dim] // parts).reshape((-1,) + (1,) * (len(dims) - 1 - dim))
    return factor_of


def bell_draw(own_key, shape, spread, reach, cuts=(), held_as=jnp.bfloat16):
    values = jax.random.normal(own_key, shape, jnp.float32) * spread
    if len(cuts) > 0:
        values = shard_levels(own_key, shape, cuts, -0.22, 0.18) * values
    return jnp.clip(values, min=-reach, max=reach).astype(held_as)


def heavy_noise(rng, dims, scale, reach, cuts, heavy, kind=jnp.bfloat16):
    result = scale * jax.random.normal(rng, dims, jnp.float32)
    if cuts:
        result = result * shard_levels(rng, dims, cuts, -0.22, 0.18)
    return jnp.clip(strengthened(result, jax.random.fold_in(rng, 3), *heavy), -reach, reach).astype(kind)


def setup_inputs(seed: int = 0) -> dict:
    seeds = jax.random.split(jax.random.key(seed), 13)
    option_latent_states = bell_draw(seeds[0], (ROWS, D), 1.0, 6.0, ((0, 8), (1, 32)))
    mixer_scaling_factor = jnp.clip(1.0 + 0.18 * jax.random.normal(seeds[1], (1, D), jnp.float32), 0.099609375, 1.8984375).astype(jnp.bfloat16)
    question_mapping_matrix = bell_draw(seeds[2], (D, HEADS * HD), D ** -0.5, 0.0625, ((1, 32),))
    lookup_content_matrix = bell_draw(seeds[3], (D, 2 * KVH * HD), D ** -0.5, 0.0625, ((1, 32),))
    final_mapping_matrix = heavy_noise(seeds[4], (HEADS * HD, D), (HEADS * HD) ** -0.5, 0.125, ((0, 32),), (0, 1, 32, 2.75))
    payoff_readout_vector = bell_draw(seeds[5], (D,), D ** -0.5, 0.0625, ((0, 32),))
    shared_trie_memo = draw_shared_trie_memo(jax.random.fold_in(seeds[12], 71), 0)
    option_route_pages = draw_option_route_pages(jax.random.fold_in(seeds[12], 71), 0)
    option_page_tally = draw_option_page_tally(jax.random.fold_in(seeds[12], 71), 0)
    option_token_span = touch_ends(jax.random.randint(seeds[9], (CANDS,), 1, STEP + 1), jax.random.fold_in(seeds[9], 1), 1, STEP).astype(jnp.int32)
    retained_pages = touch_ends(jax.random.randint(seeds[10], (N_GROUP * N_MP * RETAINED_NUMBER,), 0, LOCAL_STORE_LOAD), jax.random.fold_in(seeds[10], 1), 0, LOCAL_STORE_LOAD - 1).astype(jnp.int32)
    growth_place_mapping = draw_growth_place_mapping(jax.random.fold_in(seeds[12], 71), 0)
    return dict(option_latent_states=option_latent_states, mixer_scaling_factor=mixer_scaling_factor, question_mapping_matrix=question_mapping_matrix, lookup_content_matrix=lookup_content_matrix, final_mapping_matrix=final_mapping_matrix, payoff_readout_vector=payoff_readout_vector, shared_trie_memo=shared_trie_memo, option_route_pages=option_route_pages, option_page_tally=option_page_tally, option_token_span=option_token_span, retained_pages=retained_pages, growth_place_mapping=growth_place_mapping)


epsilon = 1e-06
masked_value = -1e+30

def rounded(values):
    return lax.optimization_barrier(values.astype(jnp.bfloat16)).astype(jnp.float32)

def attend_group(row_block, key_pool, value_pool, block_table, block_count, length, mixer_scaling_factor, question_mapping_matrix, lookup_content_matrix, final_mapping_matrix, payoff_readout_vector):
    cand_here = block_table.shape[0]
    group_size = HEADS // KVH
    rows_wide = row_block.astype(jnp.float32)
    inv_rms = lax.rsqrt(lax.optimization_barrier(jnp.mean(rows_wide * rows_wide, axis=1, keepdims=True)) + epsilon)
    scaled = (rows_wide * mixer_scaling_factor.astype(jnp.float32)).astype(jnp.bfloat16)
    queries = rounded(jnp.dot(scaled, question_mapping_matrix, preferred_element_type=jnp.float32) * inv_rms)
    fresh_pairs = rounded(jnp.dot(scaled, lookup_content_matrix, preferred_element_type=jnp.float32) * inv_rms)
    query_grid = queries.reshape(cand_here, STEP, KVH, group_size, HD)
    own_keys = fresh_pairs[:, :KVH * HD].reshape(cand_here, STEP, KVH, HD)
    own_values = fresh_pairs[:, KVH * HD:].reshape(cand_here, STEP, KVH, HD)
    path_keys = key_pool[block_table].reshape(cand_here, -1, KVH, HD).astype(jnp.float32)
    path_values = value_pool[block_table].reshape(cand_here, -1, KVH, HD).astype(jnp.float32)
    listed = jnp.arange(block_table.shape[1], dtype=jnp.int32)[None, :] < block_count[:, None]
    path_mask = jnp.repeat(listed, BLK, axis=1)
    position = jnp.arange(STEP, dtype=jnp.int32)
    own_mask = (position[None, None, :] <= position[None, :, None]) & (position[None, None, :] < length[:, None, None])
    score_scale = HD ** (-0.5)
    path_score = jnp.einsum('csgjd,cpgd->cgjsp', query_grid, path_keys) * score_scale
    own_score = jnp.einsum('csgjd,cugd->cgjsu', query_grid, own_keys) * score_scale
    path_score = jnp.where(path_mask[:, None, None, None, :], path_score, masked_value)
    own_score = jnp.where(own_mask[:, None, None, :, :], own_score, masked_value)
    row_top = jnp.maximum(lax.optimization_barrier(jnp.max(path_score, axis=-1)), lax.optimization_barrier(jnp.max(own_score, axis=-1)))
    path_mass = jnp.where(path_mask[:, None, None, None, :], jnp.exp(path_score - row_top[..., None]), 0.0)
    own_mass = jnp.where(own_mask[:, None, None, :, :], jnp.exp(own_score - row_top[..., None]), 0.0)
    row_total = lax.optimization_barrier(jnp.sum(path_mass, axis=-1)) + lax.optimization_barrier(jnp.sum(own_mass, axis=-1))
    numerator = jnp.einsum('cgjsp,cpgd->csgjd', rounded(path_mass), path_values)
    numerator = numerator + jnp.einsum('cgjsu,cugd->csgjd', rounded(own_mass), own_values)
    attended = (numerator / jnp.transpose(row_total, (0, 3, 1, 2))[..., None]).astype(jnp.bfloat16)
    attended = attended.reshape(cand_here * STEP, HEADS * HD)
    projected = jnp.dot(attended, final_mapping_matrix, preferred_element_type=jnp.float32)
    live_rows = (position[None, :] < length[:, None]).reshape(-1)
    scored = (projected * live_rows[:, None].astype(jnp.float32)).astype(jnp.bfloat16)
    last_row = (position[None, :] == length[:, None] - 1).astype(jnp.float32)
    last_values = lax.optimization_barrier(jnp.sum(projected.reshape(cand_here, STEP, -1) * last_row[:, :, None], axis=1))
    reward = lax.optimization_barrier(jnp.sum(last_values * payoff_readout_vector.astype(jnp.float32)[None, :], axis=1))
    return (scored, reward)

def reference(option_latent_states, mixer_scaling_factor, question_mapping_matrix, lookup_content_matrix, final_mapping_matrix, payoff_readout_vector, shared_trie_memo, option_route_pages, option_page_tally, option_token_span, retained_pages, growth_place_mapping):
    received = option_latent_states.reshape(N_GROUP, N_GROUP, CAND_PAIR * STEP, D)
    received = jnp.transpose(received, (1, 0, 2, 3)).reshape(N_GROUP, CAND_PAIR * N_GROUP * STEP, D)
    pool_blocks = shared_trie_memo.reshape(2, N_GROUP, LOCAL_STORE_LOAD * N_MP, BLK, KVH * HD)

    def one_group(members):
        row_block, key_pool, value_pool, block_table, block_count, length = members
        return attend_group(row_block, key_pool, value_pool, block_table, block_count, length, mixer_scaling_factor, question_mapping_matrix, lookup_content_matrix, final_mapping_matrix, payoff_readout_vector)
    scored, reward = lax.map(one_group, (received, pool_blocks[0], pool_blocks[1], option_route_pages.reshape(N_GROUP, -1, N_MP), option_page_tally.reshape(N_GROUP, -1), option_token_span.reshape(N_GROUP, -1)))
    scored = scored.reshape(-1, D)
    reward = reward.reshape(-1)
    blocks = shared_trie_memo.reshape(2, N_GROUP, N_MP, LOCAL_STORE_LOAD, BLK, KVH * HD)
    retained_page_number = retained_pages.reshape(N_GROUP, N_MP, RETAINED_NUMBER)
    place_labels = growth_place_mapping.reshape(N_GROUP, N_MP, GROWTH_PLACES)
    sender_group = place_labels // RETAINED_NUMBER
    chosen_member = place_labels % RETAINED_NUMBER
    column = jnp.broadcast_to(jnp.arange(N_MP, dtype=jnp.int32)[None, :, None], place_labels.shape)
    local_ids = retained_page_number[sender_group, column, chosen_member]
    chosen = blocks[:, sender_group, column, local_ids]
    expanded = chosen.reshape(2, N_GROUP * N_MP * GROWTH_PLACES, BLK, KVH * HD)
    return (scored, reward, expanded)
```

```python
import functools

import jax
import jax.numpy as jnp
from jax import lax
from jax.experimental import pallas as pl
from jax.experimental.pallas import tpu as pltpu
from jax.sharding import Mesh
from jax.sharding import PartitionSpec as P

D = 8192
HEADS = 64
KVH = 8
HD = 128
BLK = 128
STEP = 16
ROWS = 256
HALF = 128
EXTRA = 16
SIDE = 4
GROUPS = 8
PART = ROWS // GROUPS
SLOTS = 3
CHIPS = 16
FEAT = 256
MP = ("mp_0", "mp_1", "mp_2")
CHIP = ("mp_0", "mp_1")
GROUP_MP = ("group", "mp_0", "mp_1", "mp_2")


epsilon = 1e-06
masked_value = -1e30
MIB = 1024 * 1024

VM = pl.BlockSpec(memory_space=pltpu.VMEM)
SM = pl.BlockSpec(memory_space=pltpu.SMEM)
UNREAD = pl.BlockSpec(memory_space=pl.ANY)


def ring_shift(x, axis, by):
    size = lax.axis_size(axis)
    return lax.ppermute(x, axis, [(i, (i + by) % size) for i in range(size)])


def from_side(x, axis):
    return [x] + [ring_shift(x, axis, k) for k in (1, 2, 3)]


def call(kernel, outs, operands, specs, name, flops=1 << 22, scratch=(), room=8):
    size = sum(a.size * a.dtype.itemsize for a in outs) * 2
    return pl.pallas_call(
        kernel,
        out_shape=tuple(outs),
        in_specs=specs,
        out_specs=(VM,) * len(outs),
        scratch_shapes=scratch,
        compiler_params=pltpu.CompilerParams(vmem_limit_bytes=room * MIB),
        cost_estimate=pl.CostEstimate(flops=flops, bytes_accessed=size, transcendentals=0),
        name=name,
    )(*operands)


def shaped(*shape, dtype=jnp.bfloat16):
    return jax.ShapeDtypeStruct(shape, dtype)


def wrap(at, size):
    return lax.rem(at + size, size)


def deal_rows_kernel(where_ref, in_ref, *out_refs):
    for k, out_ref in enumerate(out_refs):
        out_ref[...] = in_ref[lax.rem(where_ref[3] + k, GROUPS)]


def deal_rows(where, states):
    return call(
        deal_rows_kernel,
        [shaped(PART, FEAT)] * GROUPS,
        (where, states.reshape(GROUPS, PART, FEAT)),
        [SM, VM],
        "deal_rows",
    )


def deal_pool_kernel(which, memo_ref, *refs):
    out_ref = refs[-1]
    for chip in range(CHIPS):
        head = chip // 2
        out_ref[chip] = memo_ref[which, :, :, head * HD : (head + 1) * HD]


def deal_pool(which, memo, after):
    return call(
        functools.partial(deal_pool_kernel, which),
        [shaped(CHIPS, 2, BLK, HD)],
        (memo, *after),
        [VM] + [UNREAD] * len(after),
        "deal_values" if which else "deal_keys",
    )[0]


def deal_final_kernel(where_ref, wo_ref, _, out_ref):
    side = lax.rem(where_ref[2] + 1, 2)
    for chip in range(CHIPS):
        place = pl.ds(pl.multiple_of((chip * 2 + side) * FEAT, FEAT), FEAT)
        out_ref[chip] = wo_ref[:, place]


def deal_final(where, wo, after):
    return call(
        deal_final_kernel,
        [shaped(CHIPS, FEAT, FEAT)],
        (where, wo, after),
        [SM, VM, UNREAD],
        "deal_final",
    )[0]


def cut_kernel(kept_ref, memo_ref, *out_refs):
    deep = BLK // GROUPS
    for entry in range(2):
        second = kept_ref[entry] == 1
        for k, out_ref in enumerate(out_refs):
            rows = slice(k * deep, (k + 1) * deep)
            for half in range(2):
                out_ref[entry, half] = jnp.where(
                    second, memo_ref[half, 1, rows], memo_ref[half, 0, rows]
                )


def cut_survivors(kept, memo, after):
    def kernel(kept_ref, memo_ref, _, *out_refs):
        cut_kernel(kept_ref, memo_ref, *out_refs)

    return call(
        kernel,
        [shaped(2, 2, BLK // GROUPS, KVH * HD)] * GROUPS,
        (kept, memo, after),
        [SM, VM, UNREAD],
        "cut_survivors",
    )


def pick_kernel(where_ref, *refs):
    labels, met, outs, held = refs[:8], refs[8:16], refs[17:25], refs[25]
    me = where_ref[3]
    for k in range(GROUPS):
        held[k] = met[k][...]
    for ahead in range(GROUPS):
        label_ref = labels[(GROUPS - ahead) % GROUPS]
        for slot in range(SLOTS):
            label = label_ref[slot]
            back = wrap(me - label // 2, GROUPS)
            outs[ahead][slot] = held[back, lax.rem(label, 2)]


def pick(where, labels, met, after):
    deep = BLK // GROUPS
    return call(
        pick_kernel,
        [shaped(SLOTS, 2, deep, KVH * HD)] * GROUPS,
        (where, *labels, *met, after),
        [SM] * 9 + [VM] * 8 + [UNREAD],
        "pick",
        scratch=[pltpu.VMEM((GROUPS, 2, 2, deep, KVH * HD), jnp.bfloat16)],
    )


def place_kernel(where_ref, label_ref, *refs):
    named, out_ref = refs[:8], refs[8]
    deep = BLK // GROUPS
    for back in range(GROUPS):
        for slot in range(SLOTS):
            source = label_ref[slot] // 2
            eighth = wrap(wrap(where_ref[3] - back, GROUPS) - source, GROUPS)
            rows = pl.ds(pl.multiple_of(eighth * deep, deep), deep)
            for half in range(2):
                out_ref[half, slot, rows, :] = named[back][slot, half]


def place(where, labels, named):
    return call(
        place_kernel,
        [shaped(2, SLOTS, BLK, KVH * HD)],
        (where, labels, *named),
        [SM, SM] + [VM] * 8,
        "place",
    )[0]


def project_kernel(where_ref, *refs):
    pieces, (wq_ref, wkv_ref, q_ref, kv_ref, pay_ref, scaled, squares) = refs[:16], refs[16:]
    upper = (pieces[0:4], pieces[8:12])
    lower = (pieces[4:8], pieces[12:16])
    y, x, core, group = where_ref[0], where_ref[1], where_ref[2], where_ref[3]
    squares[...] = jnp.zeros_like(squares)
    for other in range(2):
        source_core = lax.rem(core + other, 2)
        for back_y in range(SIDE):
            source_y = wrap(y - back_y, SIDE)
            for back_x in range(SIDE):
                source_x = wrap(x - back_x, SIDE)
                block = (source_y * SIDE + source_x) * 2 + source_core
                place = pl.ds(pl.multiple_of(block * FEAT, FEAT), FEAT)
                first = upper[other][back_y]
                second = lower[other][back_x]
                extra = first[back_x, HALF:, :].astype(jnp.float32)
                gain = extra[0:1]
                pay_ref[0:1, place] = extra[1:2]
                for k in range(GROUPS):
                    if k < GROUPS // 2:
                        piece = first[back_x, k * PART : (k + 1) * PART, :]
                    else:
                        at = k * PART - HALF
                        piece = second[back_y, at : at + PART, :]
                    rows = pl.ds(pl.multiple_of(wrap(group - k, GROUPS) * PART, PART), PART)
                    wide = piece.astype(jnp.float32)
                    scaled[rows, place] = (wide * gain).astype(jnp.bfloat16)
                    square = wide * wide
                    squares[rows, :] += square[:, :HD] + square[:, HD:]
    step = 1024

    def multiply(i, sums):
        q_sum, kv_sum = sums
        at = pl.ds(pl.multiple_of(i * step, step), step)
        part = scaled[:, at]
        q_sum += jnp.dot(part, wq_ref[at, :], preferred_element_type=jnp.float32)
        kv_sum += lax.dot_general(
            wkv_ref[:, at], part, (((1,), (1,)), ((), ())), preferred_element_type=jnp.float32
        )
        return q_sum, kv_sum

    q_sum, kv_sum = lax.fori_loop(
        0,
        D // step,
        multiply,
        (jnp.zeros((ROWS, FEAT), jnp.float32), jnp.zeros((64, ROWS), jnp.float32)),
    )
    total = squares[...]
    down = lax.rsqrt(jnp.sum(total, axis=1, keepdims=True) / D + epsilon)
    across = lax.rsqrt(jnp.sum(total.T, axis=0, keepdims=True) / D + epsilon)
    q_ref[...] = (q_sum * down).astype(jnp.bfloat16)
    kv_ref[...] = (kv_sum * across).astype(jnp.bfloat16)


def project(where, pieces, wq, wkv):
    return pl.pallas_call(
        project_kernel,
        out_shape=(
            jax.ShapeDtypeStruct((ROWS, FEAT), jnp.bfloat16),
            jax.ShapeDtypeStruct((64, ROWS), jnp.bfloat16),
            jax.ShapeDtypeStruct((1, D), jnp.float32),
        ),
        in_specs=[SM] + [VM] * 18,
        out_specs=(VM, VM, VM),
        scratch_shapes=[
            pltpu.VMEM((ROWS, D), jnp.bfloat16),
            pltpu.VMEM((ROWS, HD), jnp.float32),
        ],
        compiler_params=pltpu.CompilerParams(vmem_limit_bytes=20 * MIB),
        cost_estimate=pl.CostEstimate(
            flops=2 * ROWS * D * 320, bytes_accessed=10 << 20, transcendentals=0
        ),
        name="project",
    )(where, *pieces, wq, wkv)


def attend_kernel(
    where_ref,
    q_ref,
    near_keys,
    near_values,
    far_keys,
    far_values,
    choice_ref,
    own_ref,
    a_same,
    a_cross,
    b_same,
    b_cross,
    _,
    out_ref,
    queries,
    scores,
    tops,
    masses,
    sums,
):
    score_scale = HD ** (-0.5)
    rows = 2 * ROWS
    core, odd = where_ref[2], lax.rem(where_ref[1], 2)
    queries[:ROWS, :] = q_ref[:, :HD]
    queries[ROWS:, :] = q_ref[:, HD:]
    low, even = core == 0, odd == 0

    def put_together(same, cross):
        return jnp.concatenate(
            [jnp.where(low, same, cross), jnp.where(low, cross, same)], axis=0
        )

    first = put_together(a_same[...], a_cross[...])
    second = put_together(b_same[...], b_cross[...])
    fresh_keys = jnp.where(even, first, second)
    fresh_values = jnp.where(even, second, first)
    own_mask = own_ref[...] > 0.5
    own_mask = jnp.concatenate([own_mask, own_mask], axis=0)
    own_score = (
        jnp.dot(queries[...], fresh_keys, preferred_element_type=jnp.float32) * score_scale
    )
    own_score = jnp.where(own_mask, own_score, masked_value)
    tops[...] = jnp.maximum(own_score[:, :HD], own_score[:, HD:])

    def chosen(which):
        spread = jnp.broadcast_to(choice_ref[which][:, None, :], (ROWS // STEP, STEP, HD))
        spread = spread.reshape(ROWS, HD)
        return jnp.concatenate([spread, spread], axis=0)

    def score(i, _):
        for other, source in ((0, near_keys), (1, far_keys)):
            choice = chosen(i * 2 + lax.rem(core + other, 2))
            keys = source[i].reshape(2 * BLK, HD)
            both = lax.dot_general(
                queries[...], keys, (((1,), (1,)), ((), ())), preferred_element_type=jnp.float32
            )
            one = jnp.where(choice > 0.5, both[:, BLK:], both[:, :BLK]) * score_scale
            one = jnp.where(choice > 1.5, masked_value, one)
            scores[i * 2 + other] = one
            tops[...] = jnp.maximum(tops[...], one)
        return 0

    lax.fori_loop(0, CHIPS, score, 0)
    top = jnp.max(tops[...], axis=1, keepdims=True)
    tops[...] = jnp.broadcast_to(top, (rows, HD))
    own_mass = jnp.where(own_mask, jnp.exp(own_score - top), 0.0)
    masses[...] = own_mass[:, :HD] + own_mass[:, HD:]
    sums[...] = lax.dot_general(
        own_mass.astype(jnp.bfloat16),
        fresh_values,
        (((1,), (1,)), ((), ())),
        preferred_element_type=jnp.float32,
    )

    def weigh(i, _):
        for other, source in ((0, near_values), (1, far_values)):
            choice = chosen(i * 2 + lax.rem(core + other, 2))
            mass = jnp.exp(scores[i * 2 + other] - tops[...])
            masses[...] += mass
            weights = jnp.concatenate(
                [jnp.where(choice > 0.5, 0.0, mass), jnp.where(choice > 0.5, mass, 0.0)], axis=1
            ).astype(jnp.bfloat16)
            values = source[i].reshape(2 * BLK, HD)
            sums[...] += jnp.dot(weights, values, preferred_element_type=jnp.float32)
        return 0

    lax.fori_loop(0, CHIPS, weigh, 0)
    attended = sums[...] / jnp.sum(masses[...], axis=1, keepdims=True)
    out_ref[:, :HD] = attended[:ROWS].astype(jnp.bfloat16)
    out_ref[:, HD:] = attended[ROWS:].astype(jnp.bfloat16)


def attend(where, queries, cached, choice, own_mask, fresh, after):
    return pl.pallas_call(
        attend_kernel,
        out_shape=jax.ShapeDtypeStruct((ROWS, FEAT), jnp.bfloat16),
        in_specs=[SM] + [VM] * 11 + [UNREAD],
        out_specs=VM,
        scratch_shapes=[
            pltpu.VMEM((2 * ROWS, HD), jnp.bfloat16),
            pltpu.VMEM((2 * CHIPS, 2 * ROWS, HD), jnp.float32),
            pltpu.VMEM((2 * ROWS, HD), jnp.float32),
            pltpu.VMEM((2 * ROWS, HD), jnp.float32),
            pltpu.VMEM((2 * ROWS, HD), jnp.float32),
        ],
        compiler_params=pltpu.CompilerParams(vmem_limit_bytes=20 * MIB),
        cost_estimate=pl.CostEstimate(
            flops=8 * ROWS * 8192 * 256, bytes_accessed=5 << 20, transcendentals=ROWS * 8192
        ),
        name="attend",
    )(where, queries, *cached, choice, own_mask, *fresh, after)


def finish_kernel(where_ref, near_ref, far_ref, wo_ref, wo_far, pay_ref, *refs):
    outs, reward_ref, held = refs[:8], refs[8], refs[9]
    y, x, core = where_ref[0], where_ref[1], where_ref[2]
    reward_ref[...] = jnp.zeros_like(reward_ref)

    def multiply(i, _):
        chip = lax.rem(y + i // SIDE, SIDE) * SIDE + lax.rem(x + lax.rem(i, SIDE), SIDE)
        place = pl.ds(pl.multiple_of((chip * 2 + core) * FEAT, FEAT), FEAT)
        part = jnp.dot(near_ref[...], wo_ref[:, place], preferred_element_type=jnp.float32)
        part += jnp.dot(far_ref[...], wo_far[chip], preferred_element_type=jnp.float32)
        held[i] = part.astype(jnp.bfloat16)
        paid = part * pay_ref[0:1, place]
        reward_ref[...] += paid[:, :HD] + paid[:, HD:]
        return 0

    lax.fori_loop(0, CHIPS, multiply, 0)
    for ahead_y in range(SIDE):
        for ahead_x in range(SIDE):
            i = ahead_y * SIDE + ahead_x
            outs[ahead_x][ahead_y] = held[i, :HALF]
            outs[SIDE + ahead_y][ahead_x] = held[i, HALF:]


def finish(where, near, far, wo, wo_far, pay):
    return call(
        finish_kernel,
        [shaped(SIDE, HALF, FEAT)] * 8 + [shaped(ROWS, HD, dtype=jnp.float32)],
        (where, near, far, wo, wo_far, pay),
        [SM] + [VM] * 5,
        "finish",
        flops=2 * ROWS * 512 * 4096,
        scratch=[pltpu.VMEM((CHIPS, ROWS, FEAT), jnp.bfloat16)],
        room=16,
    )


def gather_sums_kernel(*refs):
    ins, outs = refs[:8], refs[8:]
    for half in range(2):
        for k in range(SIDE):
            total = ins[half * SIDE][k].astype(jnp.float32)
            for j in range(1, SIDE):
                total += ins[half * SIDE + j][k].astype(jnp.float32)
            outs[half * SIDE + k][...] = total.astype(jnp.bfloat16)


def gather_sums(parts):
    return call(gather_sums_kernel, [shaped(HALF, FEAT)] * 8, parts, [VM] * 8, "gather_sums")


def settle_kernel(live_ref, *refs):
    ins, out_ref = refs[:8], refs[8]
    for half in range(2):
        total = ins[half * SIDE][...].astype(jnp.float32)
        for j in range(1, SIDE):
            total += ins[half * SIDE + j][...].astype(jnp.float32)
        rows = slice(half * HALF, (half + 1) * HALF)
        out_ref[rows, :HD] = (total[:, :HD] * live_ref[rows, :]).astype(jnp.bfloat16)
        out_ref[rows, HD:] = (total[:, HD:] * live_ref[rows, :]).astype(jnp.bfloat16)


def settle(live, parts):
    return call(
        settle_kernel, [shaped(ROWS, FEAT)], (live, *parts), [VM] * 9, "settle"
    )[0]


def exchange(x, axis):
    return lax.all_to_all(x, axis, split_axis=0, concat_axis=0, tiled=True)


def shifted(blocks, axis):
    return [blocks[0]] + [ring_shift(b, axis, k) for k, b in enumerate(blocks) if k > 0]


def from_all(x, axis):
    return [x] + [ring_shift(x, axis, k) for k in range(1, lax.axis_size(axis))]


def swapped(x, axis, bit):
    size = lax.axis_size(axis)
    return lax.ppermute(x, axis, [(i, i ^ bit) for i in range(size)])


def local(
    option_latent_states,
    mixer_scaling_factor,
    question_mapping_matrix,
    lookup_content_matrix,
    final_mapping_matrix,
    payoff_readout_vector,
    shared_trie_memo,
    option_route_pages,
    option_page_tally,
    option_token_span,
    retained_pages,
    growth_place_mapping,
):
    where = jnp.stack([lax.axis_index(a) for a in (*MP, "group")]).astype(jnp.int32)
    cand_here = ROWS // STEP

    received = shifted(deal_rows(where, option_latent_states), "group")

    near_keys = exchange(deal_pool(0, shared_trie_memo, ()), CHIP)
    far_keys = swapped(near_keys, "mp_2", 1)

    extra = jnp.concatenate(
        [
            mixer_scaling_factor,
            payoff_readout_vector[None],
            jnp.zeros((EXTRA - 2, FEAT), jnp.bfloat16),
        ],
        axis=0,
    )
    upper = jnp.concatenate([*received[:4], extra], axis=0)
    lower = jnp.concatenate(received[4:], axis=0)
    upper = jnp.stack(from_side(upper, "mp_1"))
    lower = jnp.stack(from_side(lower, "mp_0"))
    pieces = from_side(upper, "mp_0") + from_side(lower, "mp_1")
    pieces = pieces + [swapped(p, "mp_2", 1) for p in pieces]

    cuts = cut_survivors(retained_pages, shared_trie_memo, received[1])
    met = shifted(cuts, "group")
    labels = from_all(growth_place_mapping, "group")

    near_values = exchange(deal_pool(1, shared_trie_memo, (upper, lower, cuts[0])), CHIP)
    far_values = swapped(near_values, "mp_2", 1)
    wo_far = swapped(deal_final(where, final_mapping_matrix, upper), "mp_2", 1)

    queries, pair_part, pay = project(
        where, pieces, question_mapping_matrix, lookup_content_matrix.T
    )

    fresh = []
    for swap in (0, 1):
        for cross in (0, 1):
            moves = []
            for h in range(KVH):
                for value in (0, 1):
                    for core in (0, 1):
                        source = (h + KVH * value) * 2 + core
                        target = (2 * h + (value ^ swap)) * 2 + (core ^ cross)
                        moves.append((source, target))
            fresh.append(lax.ppermute(pair_part, MP, moves))

    picked = pick(where, labels, met, pair_part)
    named = shifted(picked, "group")

    table = option_route_pages.shape[1]
    index = jnp.arange(table, dtype=jnp.int32)[:, None]
    choice = jnp.where(
        index < option_page_tally[None, :], option_route_pages.T - 2 * index, 2
    ).astype(jnp.float32)
    choice = jnp.broadcast_to(choice[:, :, None], (table, cand_here, HD))
    row = jnp.arange(ROWS, dtype=jnp.int32)
    span_row = jnp.broadcast_to(option_token_span[:, None], (cand_here, STEP)).reshape(ROWS)
    own_mask = (
        (row[:, None] // STEP == row[None, :] // STEP)
        & (row[None, :] <= row[:, None])
        & (row[None, :] % STEP < span_row[:, None])
    ).astype(jnp.float32)
    attended = attend(
        where,
        queries,
        (near_keys, near_values, far_keys, far_values),
        choice,
        own_mask,
        fresh,
        picked[0],
    )

    *parts, paid = finish(
        where, attended, swapped(attended, "mp_2", 1), final_mapping_matrix, wo_far, pay
    )
    parts = shifted(parts[:4], "mp_1") + shifted(parts[4:], "mp_0")
    sums = gather_sums(parts)
    sums = shifted(sums[:4], "mp_0") + shifted(sums[4:], "mp_1")
    live_rows = (row % STEP < span_row).astype(jnp.float32)
    live_rows = jnp.broadcast_to(live_rows[:, None], (ROWS, HD))
    scored_rows = settle(live_rows, sums)

    position = jnp.arange(STEP, dtype=jnp.int32)
    last_row = (position[None, :] == option_token_span[:, None] - 1).astype(jnp.float32)
    row_reward = jnp.sum(paid, axis=1).reshape(cand_here, STEP)
    rewards = jnp.sum(row_reward * last_row, axis=1)
    for axis, bit in (("mp_2", 1), ("mp_1", 1), ("mp_1", 2), ("mp_0", 1), ("mp_0", 2)):
        rewards = rewards + swapped(rewards, axis, bit)

    expanded = place(where, growth_place_mapping, named)
    return (scored_rows, rewards, expanded)


def solution(mesh):
    split = Mesh(
        mesh.devices.reshape(mesh.shape["group"], 4, 4, 2), ("group", "mp_0", "mp_1", "mp_2")
    )
    in_specs = (
        P("group", MP),
        P(None, MP),
        P(None, MP),
        P(None, MP),
        P(MP, None),
        P(MP),
        P(None, GROUP_MP, None, None),
        P("group", None),
        P("group"),
        P("group"),
        P(GROUP_MP),
        P(GROUP_MP),
    )
    out_specs = (P("group", MP), P("group"), P(None, GROUP_MP, None, None))
    return jax.shard_map(local, mesh=split, in_specs=in_specs, out_specs=out_specs, check_vma=False)
```

```python
import jax
import jax.numpy as jnp
from jax import lax
from jax.experimental import pallas as pl
from jax.experimental.pallas import tpu as pltpu
from jax.sharding import Mesh
from jax.sharding import PartitionSpec as P


D = 8192
KVH = 8
HD = 128
BLK = 128
STEP = 16
ROWS = 256
HALF = 128
EXTRA = 16
TALL = ROWS + EXTRA
GROUPS = 8
PART = ROWS // GROUPS
SIDE = 4
SLOTS = 3
CHIPS = 16
FEAT = 256
MP = ("mp_0", "mp_1", "mp_2")
CHIP = ("mp_0", "mp_1")
GROUP_MP = ("group", "mp_0", "mp_1", "mp_2")


epsilon = 1e-06
masked_value = -1e30
LOG2E = 1.4426950408889634
MIB = 1024 * 1024
ATTEND_ROOM = 40
DEAL_ROOM = 60

VM = pl.BlockSpec(memory_space=pltpu.VMEM)
SM = pl.BlockSpec(memory_space=pltpu.SMEM)
PLACE = pl.BlockSpec(memory_space=pl.ANY)


def call(kernel, outs, operands, specs, flops=1 << 22, scratch=(), room=8):
    size = sum(a.size * a.dtype.itemsize for a in outs) * 2
    return pl.pallas_call(
        kernel,
        out_shape=tuple(outs),
        in_specs=specs,
        out_specs=(VM,) * len(outs),
        scratch_shapes=scratch,
        compiler_params=pltpu.CompilerParams(vmem_limit_bytes=room * MIB),
        cost_estimate=pl.CostEstimate(flops=flops, bytes_accessed=size, transcendentals=0),
    )(*operands)


def shaped(*shape, dtype=jnp.bfloat16):
    return jax.ShapeDtypeStruct(shape, dtype)


def wrap(at, size):
    return lax.rem(at + size, size)


def deal_pool_kernel(kept_ref, memo_ref, keys_ref, values_ref, kept_out):
    for entry in range(2):
        second = kept_ref[entry] == 1
        for half in range(2):
            kept_out[entry, half] = jnp.where(second, memo_ref[half, 1], memo_ref[half, 0])
    for chip in range(CHIPS):
        lanes = slice(chip // 2 * HD, (chip // 2 + 1) * HD)
        keys_ref[chip] = memo_ref[0, :, :, lanes]
        values_ref[chip] = memo_ref[1, :, :, lanes]


def deal_pool(kept, memo):
    return call(
        deal_pool_kernel,
        [
            shaped(CHIPS, 2, BLK, HD),
            shaped(CHIPS, 2, BLK, HD),
            shaped(2, 2, BLK, KVH * HD),
        ],
        (kept, memo),
        [SM, VM],
        room=DEAL_ROOM,
    )


def ahead(core, j):
    return jnp.where(core == 0, (j + 1) % 4, 7 - j)


def deal_rows_kernel(where_ref, in_ref, extra_ref, keep_ref, give_ref):
    core, group = where_ref[2], where_ref[3]
    for j in range(4):
        keep_ref[j] = in_ref[lax.rem(group + ahead(core, j), GROUPS)]
        give_ref[j * PART : (j + 1) * PART, :] = in_ref[lax.rem(group + ahead(1 - core, j), GROUPS)]
    give_ref[HALF:, :] = extra_ref[...]


def deal_rows(where, states, extra):
    return call(
        deal_rows_kernel,
        [shaped(4, PART, FEAT), shaped(HALF + EXTRA, FEAT)],
        (where, states.reshape(GROUPS, PART, FEAT), extra),
        [SM, VM, VM],
    )


def pair_rows_kernel(keep_ref, got_ref, *out_refs):
    for j, out_ref in enumerate(out_refs):
        out_ref[0] = keep_ref[j]
        out_ref[1] = got_ref[j * PART : (j + 1) * PART, :]


def pair_rows(keep, got):
    return call(pair_rows_kernel, [shaped(2, PART, FEAT)] * 4, (keep, got), [VM, VM])


def bundle_rows_kernel(extra_ref, got_ref, *refs):
    out_ref = refs[4]
    for j in range(4):
        out_ref[:, j * PART : (j + 1) * PART, :] = refs[j][...]
    out_ref[0, HALF:, :] = extra_ref[...]
    out_ref[1, HALF:, :] = got_ref[HALF:, :]


def bundle_rows(extra, got, received):
    return call(
        bundle_rows_kernel, [shaped(2, HALF + EXTRA, FEAT)], (extra, got, *received), [VM] * 6
    )[0]


def place_kernel(label_ref, in_ref, out_ref):
    out_ref[...] = in_ref[...].reshape(out_ref.shape)


def place(labels, survivors):
    return pl.pallas_call(
        place_kernel,
        out_shape=shaped(2, SLOTS, BLK, KVH * HD),
        grid_spec=pltpu.PrefetchScalarGridSpec(
            num_scalar_prefetch=1,
            grid=(SLOTS, 2),
            in_specs=[
                pl.BlockSpec((1, 1, BLK, KVH * HD), lambda e, h, label: (label[e], h, 0, 0))
            ],
            out_specs=pl.BlockSpec((1, 1, BLK, KVH * HD), lambda e, h, label: (h, e, 0, 0)),
        ),
        compiler_params=pltpu.CompilerParams(vmem_limit_bytes=60 * MIB),
        cost_estimate=pl.CostEstimate(flops=1 << 22, bytes_accessed=3 << 20, transcendentals=0),
        name="place",
    )(labels, survivors)


def project_kernel(where_ref, *refs):
    blocks, (wq_hbm, wkv_hbm, q_ref, kv_ref, pay_ref) = refs[:8], refs[8:13]
    pieces, (wq_ref, wkv_ref, scaled, squares, sems) = refs[13:21], refs[21:]
    copies = [
        pltpu.make_async_copy(source, target, sems.at[n])
        for n, (source, target) in enumerate(
            zip((*blocks, wkv_hbm, wq_hbm), (*pieces, wkv_ref, wq_ref))
        )
    ]
    for copy in copies:
        copy.start()
    y, x, core, group = where_ref[0], where_ref[1], where_ref[2], where_ref[3]
    squares[...] = jnp.zeros_like(squares)
    for other in range(2):
        holder = core if other == 0 else 1 - core
        spots = []
        for j in range(4):
            source = wrap(group - ahead(holder, j), GROUPS)
            spots.append(pl.ds(pl.multiple_of(source * PART, PART), PART))
        for first in range(SIDE):
            copies[other * 4 + first].wait()
            piece_ref = pieces[other * 4 + first]
            for second in range(SIDE):
                back_y = jnp.where(holder == 0, first, second)
                back_x = jnp.where(holder == 0, second, first)
                chip = wrap(y - back_y, SIDE) * SIDE + wrap(x - back_x, SIDE)
                for b in range(2):
                    block = chip * 2 + (holder if b == 0 else 1 - holder)
                    place = pl.ds(pl.multiple_of(block * FEAT, FEAT), FEAT)
                    extra = piece_ref[second, b, HALF:, :].astype(jnp.float32)
                    gain = extra[0:1]
                    pay_ref[0:1, place] = extra[1:2]
                    for j in range(4):
                        rows = spots[j]
                        piece = piece_ref[second, b, j * PART : (j + 1) * PART, :]
                        wide = piece.astype(jnp.float32)
                        scaled[rows, place] = (wide * gain).astype(jnp.bfloat16)
                        square = wide * wide
                        squares[rows, :] += square[:, :HD] + square[:, HD:]
    copies[8].wait()
    copies[9].wait()
    step = 1024

    def multiply(i, sums):
        q_sum, kv_sum = sums
        at = pl.ds(pl.multiple_of(i * step, step), step)
        part = scaled[:, at]
        q_sum += jnp.dot(part, wq_ref[at, :], preferred_element_type=jnp.float32)
        kv_sum += lax.dot_general(
            part, wkv_ref[:, at], (((1,), (1,)), ((), ())), preferred_element_type=jnp.float32
        )
        return q_sum, kv_sum

    q_sum, kv_sum = lax.fori_loop(
        0,
        D // step,
        multiply,
        (jnp.zeros((ROWS, FEAT), jnp.float32), jnp.zeros((ROWS, 64), jnp.float32)),
    )
    total = squares[...]
    down = lax.rsqrt(jnp.sum(total, axis=1, keepdims=True) / D + epsilon)
    q_ref[...] = (q_sum * down).astype(jnp.bfloat16)
    kv_ref[...] = (kv_sum * down).T.astype(jnp.bfloat16)


def project(where, pieces, wq, wkv):
    return pl.pallas_call(
        project_kernel,
        out_shape=(
            jax.ShapeDtypeStruct((ROWS, FEAT), jnp.bfloat16),
            jax.ShapeDtypeStruct((64, ROWS), jnp.bfloat16),
            jax.ShapeDtypeStruct((1, D), jnp.float32),
        ),
        in_specs=[SM] + [PLACE] * 10,
        out_specs=(VM, VM, VM),
        scratch_shapes=[pltpu.VMEM(p.shape, p.dtype) for p in (*pieces, wq, wkv)]
        + [
            pltpu.VMEM((ROWS, D), jnp.bfloat16),
            pltpu.VMEM((ROWS, HD), jnp.float32),
            pltpu.SemaphoreType.DMA((10,)),
        ],
        compiler_params=pltpu.CompilerParams(vmem_limit_bytes=60 * MIB),
        cost_estimate=pl.CostEstimate(
            flops=2 * ROWS * D * 320, bytes_accessed=10 << 20, transcendentals=0
        ),
        name="project",
    )(where, *pieces, wq, wkv)


def attend_kernel(
    where_ref,
    q_ref,
    near_keys,
    far_keys,
    near_values,
    far_values,
    choice_ref,
    own_ref,
    a_same,
    a_cross,
    b_same,
    b_cross,
    keep_ref,
    give_ref,
    queries,
    scores,
    tops,
    masses,
    sums,
    near_ref,
    far_ref,
    sems,
):
    copies = []
    for n, source in enumerate((near_keys, far_keys, near_values, far_values)):
        target = (near_ref, far_ref)[n % 2]
        copies.append(pltpu.make_async_copy(source, target.at[n // 2], sems.at[n]))
        copies[n].start()
    score_scale = HD ** (-0.5) * LOG2E
    rows = 2 * ROWS
    core, odd = where_ref[2], lax.rem(where_ref[1], 2)
    queries[:ROWS, :] = q_ref[:, :HD]
    queries[ROWS:, :] = q_ref[:, HD:]
    low, even = core == 0, odd == 0

    def put_together(same, cross):
        return jnp.concatenate(
            [jnp.where(low, same, cross), jnp.where(low, cross, same)], axis=0
        )

    first = put_together(a_same[...], a_cross[...])
    second = put_together(b_same[...], b_cross[...])
    fresh_keys = jnp.where(even, first, second)
    fresh_values = jnp.where(even, second, first)
    own_mask = own_ref[...] > 0.5
    own_mask = jnp.concatenate([own_mask, own_mask], axis=0)
    own_score = (
        jnp.dot(queries[...], fresh_keys, preferred_element_type=jnp.float32) * score_scale
    )
    own_score = jnp.where(own_mask, own_score, masked_value)
    tops[...] = jnp.maximum(own_score[:, :HD], own_score[:, HD:])

    def chosen(which):
        spread = jnp.broadcast_to(choice_ref[which][:, None, :], (ROWS // STEP, STEP, HD))
        spread = spread.reshape(ROWS, HD)
        return jnp.concatenate([spread, spread], axis=0)

    def score(i, _):
        for other, source in ((0, near_ref), (1, far_ref)):
            choice = chosen(i * 2 + lax.rem(core + other, 2))
            keys = source[0, i].reshape(2 * BLK, HD)
            both = lax.dot_general(
                queries[...], keys, (((1,), (1,)), ((), ())), preferred_element_type=jnp.float32
            )
            one = jnp.where(choice > 0.5, both[:, BLK:], both[:, :BLK]) * score_scale
            one = jnp.where(choice > 1.5, masked_value, one)
            scores[i * 2 + other] = one
            tops[...] = jnp.maximum(tops[...], one)
        return 0

    copies[0].wait()
    copies[1].wait()
    lax.fori_loop(0, CHIPS, score, 0)
    top = jnp.max(tops[...], axis=1, keepdims=True)
    tops[...] = jnp.broadcast_to(top, (rows, HD))
    own_mass = jnp.where(own_mask, jnp.exp2(own_score - top), 0.0)
    masses[...] = own_mass[:, :HD] + own_mass[:, HD:]
    sums[...] = lax.dot_general(
        own_mass.astype(jnp.bfloat16),
        fresh_values,
        (((1,), (1,)), ((), ())),
        preferred_element_type=jnp.float32,
    )

    def weigh(i, _):
        for other, source in ((0, near_ref), (1, far_ref)):
            choice = chosen(i * 2 + lax.rem(core + other, 2))
            mass = jnp.exp2(scores[i * 2 + other] - tops[...])
            masses[...] += mass
            weights = jnp.concatenate(
                [jnp.where(choice > 0.5, 0.0, mass), jnp.where(choice > 0.5, mass, 0.0)], axis=1
            ).astype(jnp.bfloat16)
            values = source[1, i].reshape(2 * BLK, HD)
            sums[...] += jnp.dot(weights, values, preferred_element_type=jnp.float32)
        return 0

    copies[2].wait()
    copies[3].wait()
    lax.fori_loop(0, CHIPS, weigh, 0)
    attended = sums[...] / jnp.sum(masses[...], axis=1, keepdims=True)
    sums[...] = attended
    for mine, out_ref in ((core, keep_ref), (1 - core, give_ref)):
        for head in range(2):
            at = pl.multiple_of(head * ROWS + mine * HALF, HALF)
            out_ref[:, head * HD : (head + 1) * HD] = sums[pl.ds(at, HALF), :].astype(jnp.bfloat16)


def attend(where, queries, cached, choice, own_mask, fresh):
    return pl.pallas_call(
        attend_kernel,
        out_shape=(shaped(HALF, FEAT), shaped(HALF, FEAT)),
        in_specs=[SM, VM] + [PLACE] * 4 + [VM] * 6,
        out_specs=(VM, VM),
        scratch_shapes=[
            pltpu.VMEM((2 * ROWS, HD), jnp.bfloat16),
            pltpu.VMEM((2 * CHIPS, 2 * ROWS, HD), jnp.float32),
            pltpu.VMEM((2 * ROWS, HD), jnp.float32),
            pltpu.VMEM((2 * ROWS, HD), jnp.float32),
            pltpu.VMEM((2 * ROWS, HD), jnp.float32),
            pltpu.VMEM((2, CHIPS, 2, BLK, HD), jnp.bfloat16),
            pltpu.VMEM((2, CHIPS, 2, BLK, HD), jnp.bfloat16),
            pltpu.SemaphoreType.DMA((4,)),
        ],
        compiler_params=pltpu.CompilerParams(vmem_limit_bytes=ATTEND_ROOM * MIB),
        cost_estimate=pl.CostEstimate(
            flops=8 * ROWS * 8192 * 256, bytes_accessed=5 << 20, transcendentals=ROWS * 8192
        ),
        name="attend",
    )(where, queries, *cached, choice, own_mask, *fresh)


def in_terms(row):
    terms = []
    for _ in range(3):
        term = row.astype(jnp.bfloat16)
        row = row - term.astype(jnp.float32)
        terms.append(term.astype(jnp.float32))
    terms.append(jnp.zeros((EXTRA - 3, row.shape[1]), jnp.float32))
    return jnp.concatenate(terms, axis=0).astype(jnp.bfloat16)


def of_terms(block):
    return (block[0:1] + block[1:2]) + block[2:3]


def four(parts):
    return (parts[0] + parts[2]) + (parts[1] + parts[3])


def finish_kernel(where_ref, near_ref, far_ref, wo_ref, wo_far, pay_ref, last_ref, *refs):
    outs, reward = refs[:4], refs[4]
    y, x, core = where_ref[0], where_ref[1], where_ref[2]
    reward[...] = jnp.zeros_like(reward)
    for first in range(SIDE):
        out_ref = outs[first]

        def multiply(second, _, first=first, out_ref=out_ref):
            ahead_y = jnp.where(core == 0, second, first)
            ahead_x = jnp.where(core == 0, first, second)
            chip = lax.rem(y + ahead_y, SIDE) * SIDE + lax.rem(x + ahead_x, SIDE)
            place = pl.ds(pl.multiple_of(chip * 2 * FEAT, 2 * FEAT), 2 * FEAT)
            part = jnp.dot(near_ref[...], wo_ref[:, place], preferred_element_type=jnp.float32)
            part += jnp.dot(far_ref[...], wo_far[:, place], preferred_element_type=jnp.float32)
            out_ref[second, :HALF, :] = part[:, :FEAT].astype(jnp.bfloat16)
            out_ref[second, HALF:ROWS, :] = part[:, FEAT:].astype(jnp.bfloat16)
            paid = part * pay_ref[0:1, place]
            paid = paid[:, :FEAT] + paid[:, FEAT:]
            reward[...] += paid[:, :HD] + paid[:, HD:]
            return 0

        lax.fori_loop(0, SIDE, multiply, 0, unroll=2)
    last = jnp.where(core == 0, last_ref[:, :HALF], last_ref[:, HALF:])
    row = jnp.sum(reward[...].T, axis=0, keepdims=True) * last
    terms = in_terms(jnp.concatenate([row, jnp.zeros_like(row)], axis=1))
    for out_ref in outs:
        for second in range(SIDE):
            out_ref[second, ROWS:, :] = terms


def finish(where, near, far, wo, wo_far, pay, last_row):
    return call(
        finish_kernel,
        [shaped(SIDE, TALL, FEAT)] * SIDE,
        (where, near, far, wo, wo_far, pay, last_row),
        [SM] + [VM] * 6,
        flops=2 * ROWS * 512 * 4096,
        scratch=[pltpu.VMEM((HALF, HD), jnp.float32)],
        room=20,
    )


def add_first_kernel(*refs):
    ins, outs = refs[:4], refs[4:]
    for k, out_ref in enumerate(outs):
        for at in range(0, ROWS, 64):
            rows = slice(at, at + 64)
            total = four([ref[k, rows, :].astype(jnp.float32) for ref in ins])
            out_ref[rows, :] = total.astype(jnp.bfloat16)
        extra = four([ref[k, ROWS:, :].astype(jnp.float32) for ref in ins])
        out_ref[ROWS:, :] = in_terms(of_terms(extra))


def add_first(parts):
    return call(add_first_kernel, [shaped(TALL, FEAT)] * 4, parts, [VM] * 4)


def add_second_kernel(where_ref, live_ref, *refs):
    ins, keep_ref, give_ref, total_ref = refs[:4], refs[4], refs[5], refs[6]
    core = where_ref[2]
    live = live_ref[pl.ds(pl.multiple_of(core * HALF, HALF), HALF), :]
    live = jnp.concatenate([live, live], axis=1)
    for column in range(2):
        rows = slice(column * HALF, (column + 1) * HALF)
        total = four([ref[rows, :].astype(jnp.float32) for ref in ins])
        total_ref[column] = (total * live).astype(jnp.bfloat16)
    keep_ref[:HALF, :] = total_ref[core]
    give_ref[:HALF, :] = total_ref[1 - core]
    extra = four([ref[ROWS:, :].astype(jnp.float32) for ref in ins])
    terms = in_terms(of_terms(extra))
    keep_ref[HALF:, :] = terms
    give_ref[HALF:, :] = terms


def add_second(where, live, parts):
    return call(
        add_second_kernel,
        [shaped(HALF + EXTRA, FEAT)] * 2,
        (where, live, *parts),
        [SM] + [VM] * 5,
        scratch=[pltpu.VMEM((2, HALF, FEAT), jnp.bfloat16)],
    )


def settle_kernel(where_ref, keep_ref, got_ref, out_ref, reward_ref):
    low = where_ref[2] == 0
    upper = jnp.where(low, keep_ref[...], got_ref[...])
    lower = jnp.where(low, got_ref[...], keep_ref[...])
    out_ref[:HALF, :] = upper[:HALF]
    out_ref[HALF:, :] = lower[:HALF]
    reward_ref[:, :HALF] = of_terms(upper[HALF:].astype(jnp.float32))[:, :HALF]
    reward_ref[:, HALF:] = of_terms(lower[HALF:].astype(jnp.float32))[:, :HALF]


def settle(where, keep, got):
    return call(
        settle_kernel,
        [shaped(ROWS, FEAT), shaped(1, ROWS, dtype=jnp.float32)],
        (where, keep, got),
        [SM, VM, VM],
    )


def turned(x, first, by):
    moves = []
    for y in range(SIDE):
        for x_at in range(SIDE):
            for core in range(2):
                along_x = (core == 0) == first
                to_y = y if along_x else (y + by) % SIDE
                to_x = (x_at + by) % SIDE if along_x else x_at
                moves.append(
                    ((y * SIDE + x_at) * 2 + core, (to_y * SIDE + to_x) * 2 + core)
                )
    return lax.ppermute(x, MP, moves)


def over_groups(x, j):
    moves = []
    for group in range(GROUPS):
        for core in range(2):
            by = (j + 1) % 4 if core == 0 else 7 - j
            moves.append((group * 2 + core, (group + by) % GROUPS * 2 + core))
    return lax.ppermute(x, ("group", "mp_2"), moves)


def exchange(x, axis):
    return lax.all_to_all(x, axis, split_axis=0, concat_axis=0, tiled=True)


def swapped(x, axis, bit):
    size = lax.axis_size(axis)
    return lax.ppermute(x, axis, [(i, i ^ bit) for i in range(size)])


def local(
    option_latent_states,
    mixer_scaling_factor,
    question_mapping_matrix,
    lookup_content_matrix,
    final_mapping_matrix,
    payoff_readout_vector,
    shared_trie_memo,
    option_route_pages,
    option_page_tally,
    option_token_span,
    retained_pages,
    growth_place_mapping,
):
    where = jnp.stack([lax.axis_index(a) for a in (*MP, "group")]).astype(jnp.int32)
    cand_here = ROWS // STEP

    keys, values, survivors = deal_pool(retained_pages, shared_trie_memo)
    survivors = lax.all_gather(survivors, "group", axis=0, tiled=True)
    near_keys = exchange(keys, CHIP)
    far_keys = swapped(near_keys, "mp_2", 1)

    extra = jnp.concatenate(
        [
            mixer_scaling_factor,
            payoff_readout_vector[None],
            jnp.zeros((EXTRA - 2, FEAT), jnp.bfloat16),
        ],
        axis=0,
    )
    kept_rows, given_rows = deal_rows(where, option_latent_states, extra)
    got_rows = swapped(given_rows, "mp_2", 1)
    received = [over_groups(x, j) for j, x in enumerate(pair_rows(kept_rows, got_rows))]
    mine = bundle_rows(extra, got_rows, received)

    mine = [mine] + [turned(mine, True, k) for k in (1, 2, 3)]
    mine = jnp.stack(mine)
    pieces = [mine] + [turned(mine, False, k) for k in (1, 2, 3)]
    pieces = pieces + [swapped(p, "mp_2", 1) for p in pieces]
    near_values = exchange(values, CHIP)
    far_values = swapped(near_values, "mp_2", 1)
    wo_far = swapped(final_mapping_matrix, "mp_2", 1)

    queries, pair_part, pay = project(
        where, pieces, question_mapping_matrix, lookup_content_matrix.T
    )

    fresh = []
    for swap in (0, 1):
        moves = []
        for h in range(KVH):
            for value in (0, 1):
                moves.append((h + KVH * value, 2 * h + (value ^ swap)))
        same = lax.ppermute(pair_part, CHIP, moves)
        fresh += [same, swapped(same, "mp_2", 1)]

    table = option_route_pages.shape[1]
    index = jnp.arange(table, dtype=jnp.int32)[:, None]
    choice = jnp.where(
        index < option_page_tally[None, :], option_route_pages.T - 2 * index, 2
    ).astype(jnp.float32)
    choice = jnp.broadcast_to(choice[:, :, None], (table, cand_here, HD))
    row = jnp.arange(ROWS, dtype=jnp.int32)
    span_row = jnp.broadcast_to(option_token_span[:, None], (cand_here, STEP)).reshape(ROWS)
    own_mask = (
        (row[:, None] // STEP == row[None, :] // STEP)
        & (row[None, :] <= row[:, None])
        & (row[None, :] % STEP < span_row[:, None])
    ).astype(jnp.float32)
    kept_heads, given_heads = attend(
        where,
        queries,
        (near_keys, far_keys, near_values, far_values),
        choice,
        own_mask,
        fresh,
    )

    last_row = (row % STEP == span_row - 1).astype(jnp.float32)[None, :]
    parts = finish(
        where,
        kept_heads,
        swapped(given_heads, "mp_2", 1),
        final_mapping_matrix,
        wo_far,
        pay,
        last_row,
    )
    parts = [parts[0]] + [turned(parts[k], True, k) for k in (1, 2, 3)]
    sums = add_first(parts)
    sums = [sums[0]] + [turned(sums[k], False, k) for k in (1, 2, 3)]
    live_rows = (row % STEP < span_row).astype(jnp.float32)
    live_rows = jnp.broadcast_to(live_rows[:, None], (ROWS, HD))
    kept_sums, given_sums = add_second(where, live_rows, sums)
    scored_rows, rewards = settle(where, kept_sums, swapped(given_sums, "mp_2", 1))
    rewards = jnp.sum(rewards.reshape(cand_here, STEP), axis=1)

    expanded = place(growth_place_mapping, survivors)
    return (scored_rows, rewards, expanded)


def solution(mesh):
    split = Mesh(
        mesh.devices.reshape(mesh.shape["group"], 4, 4, 2), ("group", "mp_0", "mp_1", "mp_2")
    )
    in_specs = (
        P("group", MP),
        P(None, MP),
        P(None, MP),
        P(None, MP),
        P(MP, None),
        P(MP),
        P(None, GROUP_MP, None, None),
        P("group", None),
        P("group"),
        P("group"),
        P(GROUP_MP),
        P(GROUP_MP),
    )
    out_specs = (P("group", MP), P("group"), P(None, GROUP_MP, None, None))

    return jax.shard_map(local, mesh=split, in_specs=in_specs, out_specs=out_specs, check_vma=False)
```

```python
import jax
import jax.numpy as jnp
from jax import lax
from jax.experimental import pallas as pl
from jax.experimental.pallas import tpu as pltpu
from jax.sharding import Mesh
from jax.sharding import PartitionSpec as P


D = 8192
KVH = 8
HD = 128
BLK = 128
STEP = 16
ROWS = 256
HALF = 128
EXTRA = 16
TALL = ROWS + EXTRA
GROUPS = 8
PART = ROWS // GROUPS
SIDE = 4
SLOTS = 3
CHIPS = 16
FEAT = 256
MP = ("mp_0", "mp_1", "mp_2")
CHIP = ("mp_0", "mp_1")
GROUP_MP = ("group", "mp_0", "mp_1", "mp_2")


epsilon = 1e-06
masked_value = -1e30
LOG2E = 1.4426950408889634
MIB = 1024 * 1024
ATTEND_ROOM = 24
DEAL_ROOM = 60

VM = pl.BlockSpec(memory_space=pltpu.VMEM)
SM = pl.BlockSpec(memory_space=pltpu.SMEM)
FAR = pl.BlockSpec(memory_space=pltpu.HBM)


def call(kernel, outs, operands, specs, flops=1 << 22, scratch=(), room=8):
    size = sum(a.size * a.dtype.itemsize for a in outs) * 2
    return pl.pallas_call(
        kernel,
        out_shape=tuple(outs),
        in_specs=specs,
        out_specs=(VM,) * len(outs),
        scratch_shapes=scratch,
        compiler_params=pltpu.CompilerParams(vmem_limit_bytes=room * MIB),
        cost_estimate=pl.CostEstimate(flops=flops, bytes_accessed=size, transcendentals=0),
    )(*operands)


def shaped(*shape, dtype=jnp.bfloat16):
    return jax.ShapeDtypeStruct(shape, dtype)


def wrap(at, size):
    return lax.rem(at + size, size)


def deal_pool_kernel(kept_ref, memo_ref, keys_ref, values_ref, kept_out):
    for entry in range(2):
        second = kept_ref[entry] == 1
        for half in range(2):
            kept_out[entry, half] = jnp.where(second, memo_ref[half, 1], memo_ref[half, 0])
    for chip in range(CHIPS):
        lanes = slice(chip // 2 * HD, (chip // 2 + 1) * HD)
        keys_ref[chip] = memo_ref[0, :, :, lanes]
        values_ref[chip] = memo_ref[1, :, :, lanes]


def deal_pool(kept, memo):
    return call(
        deal_pool_kernel,
        [
            shaped(CHIPS, 2, BLK, HD),
            shaped(CHIPS, 2, BLK, HD),
            shaped(2, 2, BLK, KVH * HD),
        ],
        (kept, memo),
        [SM, VM],
        room=DEAL_ROOM,
    )


def ahead(core, j):
    return jnp.where(core == 0, (j + 1) % 4, 7 - j)


def deal_rows_kernel(where_ref, in_ref, keep_ref, give_ref):
    core, group = where_ref[2], where_ref[3]
    for j in range(4):
        keep_ref[j] = in_ref[lax.rem(group + ahead(core, j), GROUPS)]
        give_ref[j * PART : (j + 1) * PART, :] = in_ref[lax.rem(group + ahead(1 - core, j), GROUPS)]


def deal_rows(where, states):
    return call(
        deal_rows_kernel,
        [shaped(4, PART, FEAT), shaped(HALF, FEAT)],
        (where, states.reshape(GROUPS, PART, FEAT)),
        [SM, VM],
    )


def pair_rows_kernel(keep_ref, got_ref, *out_refs):
    for j, out_ref in enumerate(out_refs):
        out_ref[0] = keep_ref[j]
        out_ref[1] = got_ref[j * PART : (j + 1) * PART, :]


def pair_rows(keep, got):
    return call(pair_rows_kernel, [shaped(2, PART, FEAT)] * 4, (keep, got), [VM, VM])


def bundle_rows_kernel(extra_ref, got_ref, *refs):
    out_ref = refs[4]
    for j in range(4):
        out_ref[:, j * PART : (j + 1) * PART, :] = refs[j][...]
    out_ref[0, HALF:, :] = extra_ref[...]
    out_ref[1, HALF:, :] = got_ref[...]


def bundle_rows(extra, got, received):
    return call(
        bundle_rows_kernel, [shaped(2, HALF + EXTRA, FEAT)], (extra, got, *received), [VM] * 6
    )[0]


def marks_kernel(pages_ref, tally_ref, span_ref, choice_ref, own_ref, last_ref, live_ref):
    cands, table = pages_ref.shape

    def mark(t, _):
        for c in range(cands):
            value = jnp.where(t < tally_ref[c], pages_ref[c, t] - 2 * t, 2)
            choice_ref[t, c : c + 1, :] = jnp.full((1, HD), value, jnp.int32).astype(jnp.float32)
        return 0

    lax.fori_loop(0, table, mark, 0)
    lane = lax.broadcasted_iota(jnp.int32, (STEP, ROWS), 1)
    row = lax.broadcasted_iota(jnp.int32, (STEP, ROWS), 0)
    flat = lane[0:1]
    last = jnp.zeros((1, ROWS), jnp.float32)
    for c in range(cands):
        span = span_ref[c]
        here = lane // STEP == c
        own = here & (lane % STEP <= row) & (lane % STEP < span)
        rows = slice(c * STEP, (c + 1) * STEP)
        own_ref[rows, :] = own.astype(jnp.float32)
        last = jnp.where((flat // STEP == c) & (flat % STEP == span - 1), 1.0, last)
        live_ref[rows, :] = (row[:, :HD] < span).astype(jnp.float32)
    last_ref[...] = last


def marks(pages, tally, span):
    cands, table = pages.shape
    return call(
        marks_kernel,
        [
            shaped(table, cands, HD, dtype=jnp.float32),
            shaped(ROWS, ROWS, dtype=jnp.float32),
            shaped(1, ROWS, dtype=jnp.float32),
            shaped(ROWS, HD, dtype=jnp.float32),
        ],
        (pages, tally, span),
        [SM] * 3,
    )


def place_kernel(label_ref, in_ref, out_ref):
    out_ref[...] = in_ref[...].reshape(out_ref.shape)


def place(labels, survivors):
    return pl.pallas_call(
        place_kernel,
        out_shape=shaped(2, SLOTS, BLK, KVH * HD),
        grid_spec=pltpu.PrefetchScalarGridSpec(
            num_scalar_prefetch=1,
            grid=(SLOTS, 2),
            in_specs=[
                pl.BlockSpec((1, 1, BLK, KVH * HD), lambda e, h, label: (label[e], h, 0, 0))
            ],
            out_specs=pl.BlockSpec((1, 1, BLK, KVH * HD), lambda e, h, label: (h, e, 0, 0)),
        ),
        compiler_params=pltpu.CompilerParams(vmem_limit_bytes=60 * MIB),
        cost_estimate=pl.CostEstimate(flops=1 << 22, bytes_accessed=3 << 20, transcendentals=0),
        name="place",
    )(labels, survivors)


def project_kernel(where_ref, *refs):
    blocks, (wq_hbm, wkv_hbm, q_ref, kv_ref, pay_ref) = refs[:8], refs[8:13]
    pieces, (wq_ref, wkv_ref, scaled, squares, sems) = refs[13:21], refs[21:]
    copies = [
        pltpu.make_async_copy(source, target, sems.at[n])
        for n, (source, target) in enumerate(
            zip((*blocks, wkv_hbm, wq_hbm), (*pieces, wkv_ref, wq_ref))
        )
    ]
    for copy in copies:
        copy.start()
    y, x, core, group = where_ref[0], where_ref[1], where_ref[2], where_ref[3]
    squares[...] = jnp.zeros_like(squares)
    for other in range(2):
        holder = core if other == 0 else 1 - core
        spots = []
        for j in range(4):
            source = wrap(group - ahead(holder, j), GROUPS)
            spots.append(pl.ds(pl.multiple_of(source * PART, PART), PART))
        for first in range(SIDE):
            copies[other * 4 + first].wait()
            piece_ref = pieces[other * 4 + first]
            for second in range(SIDE):
                back_y = jnp.where(holder == 0, first, second)
                back_x = jnp.where(holder == 0, second, first)
                chip = wrap(y - back_y, SIDE) * SIDE + wrap(x - back_x, SIDE)
                for b in range(2):
                    block = chip * 2 + (holder if b == 0 else 1 - holder)
                    place = pl.ds(pl.multiple_of(block * FEAT, FEAT), FEAT)
                    extra = piece_ref[second, b, HALF:, :].astype(jnp.float32)
                    gain = extra[0:1]
                    pay_ref[0:1, place] = extra[1:2]
                    for j in range(4):
                        rows = spots[j]
                        piece = piece_ref[second, b, j * PART : (j + 1) * PART, :]
                        wide = piece.astype(jnp.float32)
                        scaled[rows, place] = (wide * gain).astype(jnp.bfloat16)
                        square = wide * wide
                        squares[rows, :] += square[:, :HD] + square[:, HD:]
    copies[8].wait()
    copies[9].wait()
    step = 1024

    def multiply(i, sums):
        q_sum, kv_sum = sums
        at = pl.ds(pl.multiple_of(i * step, step), step)
        part = scaled[:, at]
        q_sum += jnp.dot(part, wq_ref[at, :], preferred_element_type=jnp.float32)
        kv_sum += lax.dot_general(
            part, wkv_ref[:, at], (((1,), (1,)), ((), ())), preferred_element_type=jnp.float32
        )
        return q_sum, kv_sum

    q_sum, kv_sum = lax.fori_loop(
        0,
        D // step,
        multiply,
        (jnp.zeros((ROWS, FEAT), jnp.float32), jnp.zeros((ROWS, 64), jnp.float32)),
    )
    total = squares[...]
    down = lax.rsqrt(jnp.sum(total, axis=1, keepdims=True) / D + epsilon)
    q_ref[...] = (q_sum * down).astype(jnp.bfloat16)
    kv_ref[...] = (kv_sum * down).T.astype(jnp.bfloat16)


def project(where, pieces, wq, wkv):
    return pl.pallas_call(
        project_kernel,
        out_shape=(
            jax.ShapeDtypeStruct((ROWS, FEAT), jnp.bfloat16),
            jax.ShapeDtypeStruct((64, ROWS), jnp.bfloat16),
            jax.ShapeDtypeStruct((1, D), jnp.float32),
        ),
        in_specs=[SM] + [FAR] * 10,
        out_specs=(VM, VM, VM),
        scratch_shapes=[pltpu.VMEM(p.shape, p.dtype) for p in (*pieces, wq, wkv)]
        + [
            pltpu.VMEM((ROWS, D), jnp.bfloat16),
            pltpu.VMEM((ROWS, HD), jnp.float32),
            pltpu.SemaphoreType.DMA((10,)),
        ],
        compiler_params=pltpu.CompilerParams(vmem_limit_bytes=60 * MIB),
        cost_estimate=pl.CostEstimate(
            flops=2 * ROWS * D * 320, bytes_accessed=10 << 20, transcendentals=0
        ),
        name="project",
    )(where, *pieces, wq, wkv)


def attend_kernel(
    where_ref,
    q_hbm,
    near_keys,
    far_keys,
    near_values,
    far_values,
    choice_hbm,
    own_hbm,
    fresh_ref,
    fresh_far,
    keep_ref,
    give_ref,
    queries,
    scores,
    tops,
    masses,
    sums,
    near_ref,
    far_ref,
    q_ref,
    choice_ref,
    own_ref,
    sems,
):
    moves = [
        (near_keys, near_ref.at[0]),
        (far_keys, far_ref.at[0]),
        (near_values, near_ref.at[1]),
        (far_values, far_ref.at[1]),
        (q_hbm, q_ref),
        (own_hbm, own_ref),
        (choice_hbm, choice_ref),
    ]
    copies = [pltpu.make_async_copy(*move, sems.at[n]) for n, move in enumerate(moves)]
    for n in (4, 5, 6, 0, 1, 2, 3):
        copies[n].start()
    copies[4].wait()
    copies[5].wait()
    score_scale = HD ** (-0.5) * LOG2E
    rows = 2 * ROWS
    core = where_ref[2]
    queries[:ROWS, :] = q_ref[:, :HD]
    queries[ROWS:, :] = q_ref[:, HD:]
    low = core == 0
    fresh_keys = jnp.where(low, fresh_ref[...], fresh_far[...])
    fresh_values = jnp.where(low, fresh_far[...], fresh_ref[...])
    own_mask = own_ref[...] > 0.5
    own_mask = jnp.concatenate([own_mask, own_mask], axis=0)
    own_score = (
        jnp.dot(queries[...], fresh_keys, preferred_element_type=jnp.float32) * score_scale
    )
    own_score = jnp.where(own_mask, own_score, masked_value)
    tops[...] = jnp.maximum(own_score[:, :HD], own_score[:, HD:])

    def chosen(which):
        spread = jnp.broadcast_to(choice_ref[which][:, None, :], (ROWS // STEP, STEP, HD))
        spread = spread.reshape(ROWS, HD)
        return jnp.concatenate([spread, spread], axis=0)

    def score(i, _):
        for other, source in ((0, near_ref), (1, far_ref)):
            choice = chosen(i * 2 + lax.rem(core + other, 2))
            keys = source[0, i].reshape(2 * BLK, HD)
            both = lax.dot_general(
                queries[...], keys, (((1,), (1,)), ((), ())), preferred_element_type=jnp.float32
            )
            one = jnp.where(choice > 0.5, both[:, BLK:], both[:, :BLK]) * score_scale
            one = jnp.where(choice > 1.5, masked_value, one)
            scores[i * 2 + other] = one
            tops[...] = jnp.maximum(tops[...], one)
        return 0

    copies[6].wait()
    copies[0].wait()
    copies[1].wait()
    lax.fori_loop(0, CHIPS, score, 0, unroll=2)
    top = jnp.max(tops[...], axis=1, keepdims=True)
    tops[...] = jnp.broadcast_to(top, (rows, HD))
    own_mass = jnp.where(own_mask, jnp.exp2(own_score - top), 0.0)
    masses[...] = own_mass[:, :HD] + own_mass[:, HD:]
    sums[...] = lax.dot_general(
        own_mass.astype(jnp.bfloat16),
        fresh_values,
        (((1,), (1,)), ((), ())),
        preferred_element_type=jnp.float32,
    )

    def weigh(i, _):
        for other, source in ((0, near_ref), (1, far_ref)):
            choice = chosen(i * 2 + lax.rem(core + other, 2))
            mass = jnp.exp2(scores[i * 2 + other] - tops[...])
            masses[...] += mass
            weights = jnp.concatenate(
                [jnp.where(choice > 0.5, 0.0, mass), jnp.where(choice > 0.5, mass, 0.0)], axis=1
            ).astype(jnp.bfloat16)
            values = source[1, i].reshape(2 * BLK, HD)
            sums[...] += jnp.dot(weights, values, preferred_element_type=jnp.float32)
        return 0

    copies[2].wait()
    copies[3].wait()
    lax.fori_loop(0, CHIPS, weigh, 0, unroll=2)
    attended = sums[...] / jnp.sum(masses[...], axis=1, keepdims=True)
    sums[...] = attended
    for mine, out_ref in ((core, keep_ref), (1 - core, give_ref)):
        for head in range(2):
            at = pl.multiple_of(head * ROWS + mine * HALF, HALF)
            out_ref[:, head * HD : (head + 1) * HD] = sums[pl.ds(at, HALF), :].astype(jnp.bfloat16)


def attend(where, queries, cached, choice, own_mask, fresh):
    return pl.pallas_call(
        attend_kernel,
        out_shape=(shaped(HALF, FEAT), shaped(HALF, FEAT)),
        in_specs=[SM] + [FAR] * 7 + [VM] * 2,
        out_specs=(VM, VM),
        scratch_shapes=[
            pltpu.VMEM((2 * ROWS, HD), jnp.bfloat16),
            pltpu.VMEM((2 * CHIPS, 2 * ROWS, HD), jnp.float32),
            pltpu.VMEM((2 * ROWS, HD), jnp.float32),
            pltpu.VMEM((2 * ROWS, HD), jnp.float32),
            pltpu.VMEM((2 * ROWS, HD), jnp.float32),
            pltpu.VMEM((2, CHIPS, 2, BLK, HD), jnp.bfloat16),
            pltpu.VMEM((2, CHIPS, 2, BLK, HD), jnp.bfloat16),
            pltpu.VMEM((ROWS, FEAT), jnp.bfloat16),
            pltpu.VMEM(choice.shape, jnp.float32),
            pltpu.VMEM(own_mask.shape, jnp.float32),
            pltpu.SemaphoreType.DMA((7,)),
        ],
        compiler_params=pltpu.CompilerParams(vmem_limit_bytes=ATTEND_ROOM * MIB),
        cost_estimate=pl.CostEstimate(
            flops=8 * ROWS * 8192 * 256, bytes_accessed=5 << 20, transcendentals=ROWS * 8192
        ),
        name="attend",
    )(where, queries, *cached, choice, own_mask, *fresh)


def in_terms(row):
    terms = []
    for _ in range(3):
        term = row.astype(jnp.bfloat16)
        row = row - term.astype(jnp.float32)
        terms.append(term.astype(jnp.float32))
    terms.append(jnp.zeros((EXTRA - 3, row.shape[1]), jnp.float32))
    return jnp.concatenate(terms, axis=0).astype(jnp.bfloat16)


def of_terms(block):
    return (block[0:1] + block[1:2]) + block[2:3]


def four(parts):
    return (parts[0] + parts[2]) + (parts[1] + parts[3])


def finish_kernel(where_ref, near_ref, far_ref, wo_ref, wo_far, pay_ref, last_ref, *refs):
    outs, reward = refs[:4], refs[4]
    y, x, core = where_ref[0], where_ref[1], where_ref[2]
    reward[...] = jnp.zeros_like(reward)
    for first in range(SIDE):
        out_ref = outs[first]

        def multiply(second, _, first=first, out_ref=out_ref):
            ahead_y = jnp.where(core == 0, second, first)
            ahead_x = jnp.where(core == 0, first, second)
            chip = lax.rem(y + ahead_y, SIDE) * SIDE + lax.rem(x + ahead_x, SIDE)
            place = pl.ds(pl.multiple_of(chip * 2 * FEAT, 2 * FEAT), 2 * FEAT)
            part = jnp.dot(near_ref[...], wo_ref[:, place], preferred_element_type=jnp.float32)
            part += jnp.dot(far_ref[...], wo_far[:, place], preferred_element_type=jnp.float32)
            out_ref[second, :HALF, :] = part[:, :FEAT].astype(jnp.bfloat16)
            out_ref[second, HALF:ROWS, :] = part[:, FEAT:].astype(jnp.bfloat16)
            paid = part * pay_ref[0:1, place]
            paid = paid[:, :FEAT] + paid[:, FEAT:]
            reward[...] += paid[:, :HD] + paid[:, HD:]
            return 0

        lax.fori_loop(0, SIDE, multiply, 0, unroll=2)
    last = jnp.where(core == 0, last_ref[:, :HALF], last_ref[:, HALF:])
    row = jnp.sum(reward[...].T, axis=0, keepdims=True) * last
    terms = in_terms(jnp.concatenate([row, jnp.zeros_like(row)], axis=1))
    for out_ref in outs:
        for second in range(SIDE):
            out_ref[second, ROWS:, :] = terms


def finish(where, near, far, wo, wo_far, pay, last_row):
    return call(
        finish_kernel,
        [shaped(SIDE, TALL, FEAT)] * SIDE,
        (where, near, far, wo, wo_far, pay, last_row),
        [SM] + [VM] * 6,
        flops=2 * ROWS * 512 * 4096,
        scratch=[pltpu.VMEM((HALF, HD), jnp.float32)],
        room=20,
    )


def add_first_kernel(*refs):
    ins, outs = refs[:4], refs[4:]
    for k, out_ref in enumerate(outs):
        for at in range(0, ROWS, 64):
            rows = slice(at, at + 64)
            total = four([ref[k, rows, :].astype(jnp.float32) for ref in ins])
            out_ref[rows, :] = total.astype(jnp.bfloat16)
        extra = four([ref[k, ROWS:, :].astype(jnp.float32) for ref in ins])
        out_ref[ROWS:, :] = in_terms(of_terms(extra))


def add_first(parts):
    return call(add_first_kernel, [shaped(TALL, FEAT)] * 4, parts, [VM] * 4)


def add_second_kernel(where_ref, live_ref, *refs):
    ins, keep_ref, give_ref, total_ref = refs[:4], refs[4], refs[5], refs[6]
    core = where_ref[2]
    live = live_ref[pl.ds(pl.multiple_of(core * HALF, HALF), HALF), :]
    live = jnp.concatenate([live, live], axis=1)
    for column in range(2):
        rows = slice(column * HALF, (column + 1) * HALF)
        total = four([ref[rows, :].astype(jnp.float32) for ref in ins])
        total_ref[column] = (total * live).astype(jnp.bfloat16)
    keep_ref[:HALF, :] = total_ref[core]
    give_ref[:HALF, :] = total_ref[1 - core]
    extra = four([ref[ROWS:, :].astype(jnp.float32) for ref in ins])
    terms = in_terms(of_terms(extra))
    keep_ref[HALF:, :] = terms
    give_ref[HALF:, :] = terms


def add_second(where, live, parts):
    return call(
        add_second_kernel,
        [shaped(HALF + EXTRA, FEAT)] * 2,
        (where, live, *parts),
        [SM] + [VM] * 5,
        scratch=[pltpu.VMEM((2, HALF, FEAT), jnp.bfloat16)],
    )


def settle_kernel(where_ref, keep_ref, got_ref, out_ref, reward_ref):
    low = where_ref[2] == 0
    upper = jnp.where(low, keep_ref[...], got_ref[...])
    lower = jnp.where(low, got_ref[...], keep_ref[...])
    out_ref[:HALF, :] = upper[:HALF]
    out_ref[HALF:, :] = lower[:HALF]
    terms = jnp.concatenate([upper[HALF:, :HALF], lower[HALF:, :HALF]], axis=1)
    row = lax.broadcasted_iota(jnp.int32, (ROWS, HD), 0)
    lane = lax.broadcasted_iota(jnp.int32, (ROWS, HD), 1)
    member = (row // STEP == lane).astype(jnp.bfloat16)
    reward_ref[...] = of_terms(jnp.dot(terms, member, preferred_element_type=jnp.float32))


def settle(where, keep, got):
    return call(
        settle_kernel,
        [shaped(ROWS, FEAT), shaped(1, HD, dtype=jnp.float32)],
        (where, keep, got),
        [SM, VM, VM],
    )


def turned(x, first, by):
    moves = []
    for y in range(SIDE):
        for x_at in range(SIDE):
            for core in range(2):
                along_x = (core == 0) == first
                to_y = y if along_x else (y + by) % SIDE
                to_x = (x_at + by) % SIDE if along_x else x_at
                moves.append(
                    ((y * SIDE + x_at) * 2 + core, (to_y * SIDE + to_x) * 2 + core)
                )
    return lax.ppermute(x, MP, moves)


def over_groups(x, j):
    moves = []
    for group in range(GROUPS):
        for core in range(2):
            by = (j + 1) % 4 if core == 0 else 7 - j
            moves.append((group * 2 + core, (group + by) % GROUPS * 2 + core))
    return lax.ppermute(x, ("group", "mp_2"), moves)


def exchange(x, axis):
    return lax.all_to_all(x, axis, split_axis=0, concat_axis=0, tiled=True)


def swapped(x, axis, bit):
    size = lax.axis_size(axis)
    return lax.ppermute(x, axis, [(i, i ^ bit) for i in range(size)])


def local(
    option_latent_states,
    mixer_scaling_factor,
    question_mapping_matrix,
    lookup_content_matrix,
    final_mapping_matrix,
    payoff_readout_vector,
    shared_trie_memo,
    option_route_pages,
    option_page_tally,
    option_token_span,
    retained_pages,
    growth_place_mapping,
):
    where = jnp.stack([lax.axis_index(a) for a in (*MP, "group")]).astype(jnp.int32)
    cand_here = ROWS // STEP

    keys, values, survivors = deal_pool(retained_pages, shared_trie_memo)
    survivors = lax.all_gather(survivors, "group", axis=0, tiled=True)
    near_keys = exchange(keys, CHIP)
    far_keys = swapped(near_keys, "mp_2", 1)

    kept_rows, given_rows = deal_rows(where, option_latent_states)
    got_rows = swapped(given_rows, "mp_2", 1)
    received = []
    for j, x in enumerate(pair_rows(kept_rows, got_rows)):
        received.append(over_groups(x, j))
    extra = jnp.concatenate(
        [
            mixer_scaling_factor,
            payoff_readout_vector[None],
            jnp.zeros((EXTRA - 2, FEAT), jnp.bfloat16),
        ],
        axis=0,
    )
    got_extra = swapped(extra, "mp_2", 1)
    mine = bundle_rows(extra, got_extra, received)

    mine = [mine] + [turned(mine, True, k) for k in (1, 2, 3)]
    mine = jnp.stack(mine)
    pieces = [mine]
    for k in (1, 2, 3):
        pieces.append(turned(mine, False, k))
    pieces = pieces + [swapped(p, "mp_2", 1) for p in pieces]
    near_values = exchange(values, CHIP)
    far_values = swapped(near_values, "mp_2", 1)
    wo_far = swapped(final_mapping_matrix, "mp_2", 1)

    choice, own_mask, last_row, live_rows = marks(
        option_route_pages, option_page_tally, option_token_span
    )
    queries, pair_part, pay = project(
        where,
        pieces,
        question_mapping_matrix,
        lookup_content_matrix.T,
    )

    partner = swapped(pair_part, "mp_2", 1)
    low = where[2] == 0
    both = jnp.concatenate(
        [jnp.where(low, pair_part, partner), jnp.where(low, partner, pair_part)], axis=0
    )
    moves = []
    for h in range(KVH):
        for value in (0, 1):
            for odd in (0, 1):
                moves.append(((h + KVH * value) * 2 + odd, (2 * h + odd) * 2 + value))
    fresh = lax.ppermute(both, MP, moves)
    fresh_far = swapped(fresh, "mp_2", 1)

    kept_heads, given_heads = attend(
        where,
        queries,
        (near_keys, far_keys, near_values, far_values),
        choice,
        own_mask,
        (fresh, fresh_far),
    )

    parts = finish(
        where,
        kept_heads,
        swapped(given_heads, "mp_2", 1),
        final_mapping_matrix,
        wo_far,
        pay,
        last_row,
    )
    moved = [parts[0]]
    for k in (1, 2, 3):
        moved.append(turned(parts[k], True, k))
    sums = add_first(moved)
    sums = [sums[0]] + [turned(sums[k], False, k) for k in (1, 2, 3)]
    kept_sums, given_sums = add_second(where, live_rows, sums)
    scored_rows, rewards = settle(where, kept_sums, swapped(given_sums, "mp_2", 1))
    rewards = rewards[0, :cand_here]

    expanded = place(growth_place_mapping, survivors)
    return (scored_rows, rewards, expanded)


def solution(mesh):
    split = Mesh(
        mesh.devices.reshape(mesh.shape["group"], 4, 4, 2), ("group", "mp_0", "mp_1", "mp_2")
    )
    in_specs = (
        P("group", MP),
        P(None, MP),
        P(None, MP),
        P(None, MP),
        P(MP, None),
        P(MP),
        P(None, GROUP_MP, None, None),
        P("group", None),
        P("group"),
        P("group"),
        P(GROUP_MP),
        P(GROUP_MP),
    )
    out_specs = (P("group", MP), P("group"), P(None, GROUP_MP, None, None))

    return jax.shard_map(local, mesh=split, in_specs=in_specs, out_specs=out_specs, check_vma=False)
```

```python
import jax
import jax.numpy as jnp
from jax import lax
from jax.experimental import pallas as pl
from jax.experimental.pallas import tpu as pltpu
from jax.sharding import Mesh
from jax.sharding import PartitionSpec as P


D = 8192
KVH = 8
HD = 128
BLK = 128
STEP = 16
ROWS = 256
HALF = 128
EXTRA = 16
TALL = ROWS + EXTRA
GROUPS = 8
PART = ROWS // GROUPS
SIDE = 4
SLOTS = 3
CHIPS = 16
FEAT = 256
MP = ("mp_0", "mp_1", "mp_2")
CHIP = ("mp_0", "mp_1")
GROUP_MP = ("group", "mp_0", "mp_1", "mp_2")


epsilon = 1e-06
masked_value = -1e30
LOG2E = 1.4426950408889634
MIB = 1024 * 1024
ATTEND_ROOM = 24
DEAL_ROOM = 60

VM = pl.BlockSpec(memory_space=pltpu.VMEM)
SM = pl.BlockSpec(memory_space=pltpu.SMEM)
FAR = pl.BlockSpec(memory_space=pltpu.HBM)


def call(kernel, outs, operands, specs, flops=1 << 22, scratch=(), room=8):
    size = sum(a.size * a.dtype.itemsize for a in outs) * 2
    return pl.pallas_call(
        kernel,
        out_shape=tuple(outs),
        in_specs=specs,
        out_specs=(VM,) * len(outs),
        scratch_shapes=scratch,
        compiler_params=pltpu.CompilerParams(vmem_limit_bytes=room * MIB),
        cost_estimate=pl.CostEstimate(flops=flops, bytes_accessed=size, transcendentals=0),
    )(*operands)


def shaped(*shape, dtype=jnp.bfloat16):
    return jax.ShapeDtypeStruct(shape, dtype)


def wrap(at, size):
    return lax.rem(at + size, size)


def deal_pool_kernel(kept_ref, memo_ref, keys_ref, values_ref, kept_out):
    for entry in range(2):
        second = kept_ref[entry] == 1
        for half in range(2):
            kept_out[entry, half] = jnp.where(second, memo_ref[half, 1], memo_ref[half, 0])
    for chip in range(CHIPS):
        lanes = slice(chip // 2 * HD, (chip // 2 + 1) * HD)
        keys_ref[chip] = memo_ref[0, :, :, lanes]
        values_ref[chip] = memo_ref[1, :, :, lanes]


def deal_pool(kept, memo):
    return call(
        deal_pool_kernel,
        [
            shaped(CHIPS, 2, BLK, HD),
            shaped(CHIPS, 2, BLK, HD),
            shaped(2, 2, BLK, KVH * HD),
        ],
        (kept, memo),
        [SM, VM],
        room=DEAL_ROOM,
    )


def ahead(core, j):
    return jnp.where(core == 0, (j + 1) % 4, 7 - j)


def deal_rows_kernel(where_ref, in_ref, keep_ref, give_ref):
    core, group = where_ref[2], where_ref[3]
    for j in range(4):
        keep_ref[j] = in_ref[lax.rem(group + ahead(core, j), GROUPS)]
        give_ref[j * PART : (j + 1) * PART, :] = in_ref[lax.rem(group + ahead(1 - core, j), GROUPS)]


def deal_rows(where, states):
    return call(
        deal_rows_kernel,
        [shaped(4, PART, FEAT), shaped(HALF, FEAT)],
        (where, states.reshape(GROUPS, PART, FEAT)),
        [SM, VM],
    )


def pair_rows_kernel(keep_ref, got_ref, *out_refs):
    for j, out_ref in enumerate(out_refs):
        out_ref[0] = keep_ref[j]
        out_ref[1] = got_ref[j * PART : (j + 1) * PART, :]


def pair_rows(keep, got):
    return call(pair_rows_kernel, [shaped(2, PART, FEAT)] * 4, (keep, got), [VM, VM])


def bundle_rows_kernel(extra_ref, got_ref, *refs):
    out_ref = refs[4]
    for j in range(4):
        out_ref[:, j * PART : (j + 1) * PART, :] = refs[j][...]
    out_ref[0, HALF:, :] = extra_ref[...]
    out_ref[1, HALF:, :] = got_ref[...]


def bundle_rows(extra, got, received):
    return call(
        bundle_rows_kernel, [shaped(2, HALF + EXTRA, FEAT)], (extra, got, *received), [VM] * 6
    )[0]


def marks_kernel(pages_ref, tally_ref, span_ref, choice_ref, own_ref, last_ref, live_ref):
    cands, table = pages_ref.shape

    def mark(t, _):
        for c in range(cands):
            value = jnp.where(t < tally_ref[c], pages_ref[c, t] - 2 * t, 2)
            choice_ref[t, c : c + 1, :] = jnp.full((1, HD), value, jnp.int32).astype(jnp.float32)
        return 0

    lax.fori_loop(0, table, mark, 0)
    lane = lax.broadcasted_iota(jnp.int32, (STEP, ROWS), 1)
    row = lax.broadcasted_iota(jnp.int32, (STEP, ROWS), 0)
    flat = lane[0:1]
    last = jnp.zeros((1, ROWS), jnp.float32)
    for c in range(cands):
        span = span_ref[c]
        here = lane // STEP == c
        own = here & (lane % STEP <= row) & (lane % STEP < span)
        rows = slice(c * STEP, (c + 1) * STEP)
        own_ref[rows, :] = own.astype(jnp.float32)
        last = jnp.where((flat // STEP == c) & (flat % STEP == span - 1), 1.0, last)
        live_ref[rows, :] = (row[:, :HD] < span).astype(jnp.float32)
    last_ref[...] = last


def marks(pages, tally, span):
    cands, table = pages.shape
    return call(
        marks_kernel,
        [
            shaped(table, cands, HD, dtype=jnp.float32),
            shaped(ROWS, ROWS, dtype=jnp.float32),
            shaped(1, ROWS, dtype=jnp.float32),
            shaped(ROWS, HD, dtype=jnp.float32),
        ],
        (pages, tally, span),
        [SM] * 3,
    )


def place_kernel(label_ref, in_ref, out_ref):
    out_ref[...] = in_ref[...].reshape(out_ref.shape)


def place(labels, survivors):
    return pl.pallas_call(
        place_kernel,
        out_shape=shaped(2, SLOTS, BLK, KVH * HD),
        grid_spec=pltpu.PrefetchScalarGridSpec(
            num_scalar_prefetch=1,
            grid=(SLOTS, 2),
            in_specs=[
                pl.BlockSpec((1, 1, BLK, KVH * HD), lambda e, h, label: (label[e], h, 0, 0))
            ],
            out_specs=pl.BlockSpec((1, 1, BLK, KVH * HD), lambda e, h, label: (h, e, 0, 0)),
        ),
        compiler_params=pltpu.CompilerParams(vmem_limit_bytes=60 * MIB),
        cost_estimate=pl.CostEstimate(flops=1 << 22, bytes_accessed=3 << 20, transcendentals=0),
        name="place",
    )(labels, survivors)


def project_kernel(where_ref, *refs):
    blocks, (wq_hbm, wkv_hbm, q_ref, kv_ref, pay_ref) = refs[:8], refs[8:13]
    pieces, (wq_ref, wkv_ref, scaled, squares, sems) = refs[13:21], refs[21:]
    copies = [
        pltpu.make_async_copy(source, target, sems.at[n])
        for n, (source, target) in enumerate(
            zip((*blocks, wkv_hbm, wq_hbm), (*pieces, wkv_ref, wq_ref))
        )
    ]
    for copy in copies:
        copy.start()
    y, x, core, group = where_ref[0], where_ref[1], where_ref[2], where_ref[3]
    squares[...] = jnp.zeros_like(squares)
    for other in range(2):
        holder = core if other == 0 else 1 - core
        spots = []
        for j in range(4):
            source = wrap(group - ahead(holder, j), GROUPS)
            spots.append(pl.ds(pl.multiple_of(source * PART, PART), PART))
        for first in range(SIDE):
            copies[other * 4 + first].wait()
            piece_ref = pieces[other * 4 + first]
            for second in range(SIDE):
                back_y = jnp.where(holder == 0, first, second)
                back_x = jnp.where(holder == 0, second, first)
                chip = wrap(y - back_y, SIDE) * SIDE + wrap(x - back_x, SIDE)
                for b in range(2):
                    block = chip * 2 + (holder if b == 0 else 1 - holder)
                    place = pl.ds(pl.multiple_of(block * FEAT, FEAT), FEAT)
                    extra = piece_ref[second, b, HALF:, :].astype(jnp.float32)
                    gain = extra[0:1]
                    pay_ref[0:1, place] = extra[1:2]
                    for j in range(4):
                        rows = spots[j]
                        piece = piece_ref[second, b, j * PART : (j + 1) * PART, :]
                        wide = piece.astype(jnp.float32)
                        scaled[rows, place] = (wide * gain).astype(jnp.bfloat16)
                        square = wide * wide
                        squares[rows, :] += square[:, :HD] + square[:, HD:]
    copies[8].wait()
    copies[9].wait()
    step = 1024

    def multiply(i, sums):
        q_sum, kv_sum = sums
        at = pl.ds(pl.multiple_of(i * step, step), step)
        part = scaled[:, at]
        q_sum += jnp.dot(part, wq_ref[at, :], preferred_element_type=jnp.float32)
        kv_sum += lax.dot_general(
            part, wkv_ref[:, at], (((1,), (1,)), ((), ())), preferred_element_type=jnp.float32
        )
        return q_sum, kv_sum

    q_sum, kv_sum = lax.fori_loop(
        0,
        D // step,
        multiply,
        (jnp.zeros((ROWS, FEAT), jnp.float32), jnp.zeros((ROWS, 64), jnp.float32)),
        unroll=4,
    )
    total = squares[...]
    down = lax.rsqrt(jnp.sum(total, axis=1, keepdims=True) / D + epsilon)
    q_ref[...] = (q_sum * down).astype(jnp.bfloat16)
    kv_ref[...] = (kv_sum * down).T.astype(jnp.bfloat16)


def project(where, pieces, wq, wkv):
    return pl.pallas_call(
        project_kernel,
        out_shape=(
            jax.ShapeDtypeStruct((ROWS, FEAT), jnp.bfloat16),
            jax.ShapeDtypeStruct((64, ROWS), jnp.bfloat16),
            jax.ShapeDtypeStruct((1, D), jnp.float32),
        ),
        in_specs=[SM] + [FAR] * 10,
        out_specs=(VM, VM, VM),
        scratch_shapes=[pltpu.VMEM(p.shape, p.dtype) for p in (*pieces, wq, wkv)]
        + [
            pltpu.VMEM((ROWS, D), jnp.bfloat16),
            pltpu.VMEM((ROWS, HD), jnp.float32),
            pltpu.SemaphoreType.DMA((10,)),
        ],
        compiler_params=pltpu.CompilerParams(vmem_limit_bytes=60 * MIB),
        cost_estimate=pl.CostEstimate(
            flops=2 * ROWS * D * 320, bytes_accessed=10 << 20, transcendentals=0
        ),
        name="project",
    )(where, *pieces, wq, wkv)


def attend_kernel(
    where_ref,
    q_hbm,
    near_keys,
    far_keys,
    near_values,
    far_values,
    choice_hbm,
    own_hbm,
    fresh_ref,
    fresh_far,
    keep_ref,
    give_ref,
    queries,
    scores,
    tops,
    masses,
    sums,
    near_ref,
    far_ref,
    q_ref,
    choice_ref,
    own_ref,
    sems,
):
    moves = [
        (near_keys, near_ref.at[0]),
        (far_keys, far_ref.at[0]),
        (near_values, near_ref.at[1]),
        (far_values, far_ref.at[1]),
        (q_hbm, q_ref),
        (own_hbm, own_ref),
        (choice_hbm, choice_ref),
    ]
    copies = [pltpu.make_async_copy(*move, sems.at[n]) for n, move in enumerate(moves)]
    for n in (4, 5, 6, 0, 1, 2, 3):
        copies[n].start()
    copies[4].wait()
    copies[5].wait()
    score_scale = HD ** (-0.5) * LOG2E
    rows = 2 * ROWS
    core = where_ref[2]
    queries[:ROWS, :] = q_ref[:, :HD]
    queries[ROWS:, :] = q_ref[:, HD:]
    low = core == 0
    fresh_keys = jnp.where(low, fresh_ref[...], fresh_far[...])
    fresh_values = jnp.where(low, fresh_far[...], fresh_ref[...])
    own_mask = own_ref[...] > 0.5
    own_mask = jnp.concatenate([own_mask, own_mask], axis=0)
    own_score = (
        jnp.dot(queries[...], fresh_keys, preferred_element_type=jnp.float32) * score_scale
    )
    own_score = jnp.where(own_mask, own_score, masked_value)
    tops[...] = jnp.maximum(own_score[:, :HD], own_score[:, HD:])

    def chosen(which):
        spread = jnp.broadcast_to(choice_ref[which][:, None, :], (ROWS // STEP, STEP, HD))
        spread = spread.reshape(ROWS, HD)
        return jnp.concatenate([spread, spread], axis=0)

    def score(i, _):
        for other, source in ((0, near_ref), (1, far_ref)):
            choice = chosen(i * 2 + lax.rem(core + other, 2))
            keys = source[0, i].reshape(2 * BLK, HD)
            both = lax.dot_general(
                queries[...], keys, (((1,), (1,)), ((), ())), preferred_element_type=jnp.float32
            )
            one = jnp.where(choice > 0.5, both[:, BLK:], both[:, :BLK]) * score_scale
            one = jnp.where(choice > 1.5, masked_value, one)
            scores[i * 2 + other] = one
            tops[...] = jnp.maximum(tops[...], one)
        return 0

    copies[6].wait()
    copies[0].wait()
    copies[1].wait()
    lax.fori_loop(0, CHIPS, score, 0, unroll=16)
    top = jnp.max(tops[...], axis=1, keepdims=True)
    tops[...] = jnp.broadcast_to(top, (rows, HD))
    own_mass = jnp.where(own_mask, jnp.exp2(own_score - top), 0.0)
    masses[...] = own_mass[:, :HD] + own_mass[:, HD:]
    sums[...] = lax.dot_general(
        own_mass.astype(jnp.bfloat16),
        fresh_values,
        (((1,), (1,)), ((), ())),
        preferred_element_type=jnp.float32,
    )

    def weigh(i, _):
        for other, source in ((0, near_ref), (1, far_ref)):
            choice = chosen(i * 2 + lax.rem(core + other, 2))
            mass = jnp.exp2(scores[i * 2 + other] - tops[...])
            masses[...] += mass
            weights = jnp.concatenate(
                [jnp.where(choice > 0.5, 0.0, mass), jnp.where(choice > 0.5, mass, 0.0)], axis=1
            ).astype(jnp.bfloat16)
            values = source[1, i].reshape(2 * BLK, HD)
            sums[...] += jnp.dot(weights, values, preferred_element_type=jnp.float32)
        return 0

    copies[2].wait()
    copies[3].wait()
    lax.fori_loop(0, CHIPS, weigh, 0, unroll=16)
    attended = sums[...] / jnp.sum(masses[...], axis=1, keepdims=True)
    sums[...] = attended
    for mine, out_ref in ((core, keep_ref), (1 - core, give_ref)):
        for head in range(2):
            at = pl.multiple_of(head * ROWS + mine * HALF, HALF)
            out_ref[:, head * HD : (head + 1) * HD] = sums[pl.ds(at, HALF), :].astype(jnp.bfloat16)


def attend(where, queries, cached, choice, own_mask, fresh):
    return pl.pallas_call(
        attend_kernel,
        out_shape=(shaped(HALF, FEAT), shaped(HALF, FEAT)),
        in_specs=[SM] + [FAR] * 7 + [VM] * 2,
        out_specs=(VM, VM),
        scratch_shapes=[
            pltpu.VMEM((2 * ROWS, HD), jnp.bfloat16),
            pltpu.VMEM((2 * CHIPS, 2 * ROWS, HD), jnp.float32),
            pltpu.VMEM((2 * ROWS, HD), jnp.float32),
            pltpu.VMEM((2 * ROWS, HD), jnp.float32),
            pltpu.VMEM((2 * ROWS, HD), jnp.float32),
            pltpu.VMEM((2, CHIPS, 2, BLK, HD), jnp.bfloat16),
            pltpu.VMEM((2, CHIPS, 2, BLK, HD), jnp.bfloat16),
            pltpu.VMEM((ROWS, FEAT), jnp.bfloat16),
            pltpu.VMEM(choice.shape, jnp.float32),
            pltpu.VMEM(own_mask.shape, jnp.float32),
            pltpu.SemaphoreType.DMA((7,)),
        ],
        compiler_params=pltpu.CompilerParams(vmem_limit_bytes=ATTEND_ROOM * MIB),
        cost_estimate=pl.CostEstimate(
            flops=8 * ROWS * 8192 * 256, bytes_accessed=5 << 20, transcendentals=ROWS * 8192
        ),
        name="attend",
    )(where, queries, *cached, choice, own_mask, *fresh)


def in_terms(row):
    terms = []
    for _ in range(3):
        term = row.astype(jnp.bfloat16)
        row = row - term.astype(jnp.float32)
        terms.append(term.astype(jnp.float32))
    terms.append(jnp.zeros((EXTRA - 3, row.shape[1]), jnp.float32))
    return jnp.concatenate(terms, axis=0).astype(jnp.bfloat16)


def of_terms(block):
    return (block[0:1] + block[1:2]) + block[2:3]


def four(parts):
    return (parts[0] + parts[2]) + (parts[1] + parts[3])


def finish_kernel(where_ref, near_ref, far_ref, wo_ref, wo_far, pay_ref, last_ref, *refs):
    outs, reward = refs[:4], refs[4]
    y, x, core = where_ref[0], where_ref[1], where_ref[2]
    reward[...] = jnp.zeros_like(reward)
    for first in range(SIDE):
        out_ref = outs[first]

        def multiply(second, _, first=first, out_ref=out_ref):
            ahead_y = jnp.where(core == 0, second, first)
            ahead_x = jnp.where(core == 0, first, second)
            chip = lax.rem(y + ahead_y, SIDE) * SIDE + lax.rem(x + ahead_x, SIDE)
            place = pl.ds(pl.multiple_of(chip * 2 * FEAT, 2 * FEAT), 2 * FEAT)
            part = jnp.dot(near_ref[...], wo_ref[:, place], preferred_element_type=jnp.float32)
            part += jnp.dot(far_ref[...], wo_far[:, place], preferred_element_type=jnp.float32)
            out_ref[second, :HALF, :] = part[:, :FEAT].astype(jnp.bfloat16)
            out_ref[second, HALF:ROWS, :] = part[:, FEAT:].astype(jnp.bfloat16)
            paid = part * pay_ref[0:1, place]
            paid = paid[:, :FEAT] + paid[:, FEAT:]
            reward[...] += paid[:, :HD] + paid[:, HD:]
            return 0

        lax.fori_loop(0, SIDE, multiply, 0, unroll=4)
    last = jnp.where(core == 0, last_ref[:, :HALF], last_ref[:, HALF:])
    row = jnp.sum(reward[...].T, axis=0, keepdims=True) * last
    terms = in_terms(jnp.concatenate([row, jnp.zeros_like(row)], axis=1))
    for out_ref in outs:
        for second in range(SIDE):
            out_ref[second, ROWS:, :] = terms


def finish(where, near, far, wo, wo_far, pay, last_row):
    return call(
        finish_kernel,
        [shaped(SIDE, TALL, FEAT)] * SIDE,
        (where, near, far, wo, wo_far, pay, last_row),
        [SM] + [VM] * 6,
        flops=2 * ROWS * 512 * 4096,
        scratch=[pltpu.VMEM((HALF, HD), jnp.float32)],
        room=20,
    )


def add_first_kernel(*refs):
    ins, outs = refs[:4], refs[4:]
    for k, out_ref in enumerate(outs):
        for at in range(0, ROWS, 64):
            rows = slice(at, at + 64)
            total = four([ref[k, rows, :].astype(jnp.float32) for ref in ins])
            out_ref[rows, :] = total.astype(jnp.bfloat16)
        extra = four([ref[k, ROWS:, :].astype(jnp.float32) for ref in ins])
        out_ref[ROWS:, :] = in_terms(of_terms(extra))


def add_first(parts):
    return call(add_first_kernel, [shaped(TALL, FEAT)] * 4, parts, [VM] * 4)


def add_second_kernel(where_ref, live_ref, *refs):
    ins, keep_ref, give_ref, total_ref = refs[:4], refs[4], refs[5], refs[6]
    core = where_ref[2]
    live = live_ref[pl.ds(pl.multiple_of(core * HALF, HALF), HALF), :]
    live = jnp.concatenate([live, live], axis=1)
    for column in range(2):
        rows = slice(column * HALF, (column + 1) * HALF)
        total = four([ref[rows, :].astype(jnp.float32) for ref in ins])
        total_ref[column] = (total * live).astype(jnp.bfloat16)
    keep_ref[:HALF, :] = total_ref[core]
    give_ref[:HALF, :] = total_ref[1 - core]
    extra = four([ref[ROWS:, :].astype(jnp.float32) for ref in ins])
    terms = in_terms(of_terms(extra))
    keep_ref[HALF:, :] = terms
    give_ref[HALF:, :] = terms


def add_second(where, live, parts):
    return call(
        add_second_kernel,
        [shaped(HALF + EXTRA, FEAT)] * 2,
        (where, live, *parts),
        [SM] + [VM] * 5,
        scratch=[pltpu.VMEM((2, HALF, FEAT), jnp.bfloat16)],
    )


def settle_kernel(where_ref, keep_ref, got_ref, out_ref, reward_ref):
    low = where_ref[2] == 0
    upper = jnp.where(low, keep_ref[...], got_ref[...])
    lower = jnp.where(low, got_ref[...], keep_ref[...])
    out_ref[:HALF, :] = upper[:HALF]
    out_ref[HALF:, :] = lower[:HALF]
    terms = jnp.concatenate([upper[HALF:, :HALF], lower[HALF:, :HALF]], axis=1)
    row = lax.broadcasted_iota(jnp.int32, (ROWS, HD), 0)
    lane = lax.broadcasted_iota(jnp.int32, (ROWS, HD), 1)
    member = (row // STEP == lane).astype(jnp.bfloat16)
    reward_ref[...] = of_terms(jnp.dot(terms, member, preferred_element_type=jnp.float32))


def settle(where, keep, got):
    return call(
        settle_kernel,
        [shaped(ROWS, FEAT), shaped(1, HD, dtype=jnp.float32)],
        (where, keep, got),
        [SM, VM, VM],
    )


def turned(x, first, by):
    moves = []
    for y in range(SIDE):
        for x_at in range(SIDE):
            for core in range(2):
                along_x = (core == 0) == first
                to_y = y if along_x else (y + by) % SIDE
                to_x = (x_at + by) % SIDE if along_x else x_at
                moves.append(
                    ((y * SIDE + x_at) * 2 + core, (to_y * SIDE + to_x) * 2 + core)
                )
    return lax.ppermute(x, MP, moves)


def over_groups(x, j):
    moves = []
    for group in range(GROUPS):
        for core in range(2):
            by = (j + 1) % 4 if core == 0 else 7 - j
            moves.append((group * 2 + core, (group + by) % GROUPS * 2 + core))
    return lax.ppermute(x, ("group", "mp_2"), moves)


def exchange(x, axis):
    return lax.all_to_all(x, axis, split_axis=0, concat_axis=0, tiled=True)


def swapped(x, axis, bit):
    size = lax.axis_size(axis)
    return lax.ppermute(x, axis, [(i, i ^ bit) for i in range(size)])


def local(
    option_latent_states,
    mixer_scaling_factor,
    question_mapping_matrix,
    lookup_content_matrix,
    final_mapping_matrix,
    payoff_readout_vector,
    shared_trie_memo,
    option_route_pages,
    option_page_tally,
    option_token_span,
    retained_pages,
    growth_place_mapping,
):
    where = jnp.stack([lax.axis_index(a) for a in (*MP, "group")]).astype(jnp.int32)
    cand_here = ROWS // STEP

    keys, values, survivors = deal_pool(retained_pages, shared_trie_memo)
    survivors = lax.all_gather(survivors, "group", axis=0, tiled=True)
    near_keys = exchange(keys, CHIP)
    far_keys = swapped(near_keys, "mp_2", 1)

    kept_rows, given_rows = deal_rows(where, option_latent_states)
    got_rows = swapped(given_rows, "mp_2", 1)
    received = []
    for j, x in enumerate(pair_rows(kept_rows, got_rows)):
        received.append(over_groups(x, j))
    extra = jnp.concatenate(
        [
            mixer_scaling_factor,
            payoff_readout_vector[None],
            jnp.zeros((EXTRA - 2, FEAT), jnp.bfloat16),
        ],
        axis=0,
    )
    got_extra = swapped(extra, "mp_2", 1)
    mine = bundle_rows(extra, got_extra, received)

    mine = [mine] + [turned(mine, True, k) for k in (1, 2, 3)]
    mine = jnp.stack(mine)
    pieces = [mine]
    for k in (1, 2, 3):
        pieces.append(turned(mine, False, k))
    pieces = pieces + [swapped(p, "mp_2", 1) for p in pieces]
    near_values = exchange(values, CHIP)
    far_values = swapped(near_values, "mp_2", 1)
    wo_far = swapped(final_mapping_matrix, "mp_2", 1)

    choice, own_mask, last_row, live_rows = marks(
        option_route_pages, option_page_tally, option_token_span
    )
    queries, pair_part, pay = project(
        where,
        pieces,
        question_mapping_matrix,
        lookup_content_matrix.T,
    )

    partner = swapped(pair_part, "mp_2", 1)
    low = where[2] == 0
    both = jnp.concatenate(
        [jnp.where(low, pair_part, partner), jnp.where(low, partner, pair_part)], axis=0
    )
    moves = []
    for h in range(KVH):
        for value in (0, 1):
            for odd in (0, 1):
                moves.append(((h + KVH * value) * 2 + odd, (2 * h + odd) * 2 + value))
    fresh = lax.ppermute(both, MP, moves)
    fresh_far = swapped(fresh, "mp_2", 1)

    kept_heads, given_heads = attend(
        where,
        queries,
        (near_keys, far_keys, near_values, far_values),
        choice,
        own_mask,
        (fresh, fresh_far),
    )

    parts = finish(
        where,
        kept_heads,
        swapped(given_heads, "mp_2", 1),
        final_mapping_matrix,
        wo_far,
        pay,
        last_row,
    )
    moved = [parts[0]]
    for k in (1, 2, 3):
        moved.append(turned(parts[k], True, k))
    sums = add_first(moved)
    sums = [sums[0]] + [turned(sums[k], False, k) for k in (1, 2, 3)]
    kept_sums, given_sums = add_second(where, live_rows, sums)
    scored_rows, rewards = settle(where, kept_sums, swapped(given_sums, "mp_2", 1))
    rewards = rewards[0, :cand_here]

    expanded = place(growth_place_mapping, survivors)
    return (scored_rows, rewards, expanded)


def solution(mesh):
    split = Mesh(
        mesh.devices.reshape(mesh.shape["group"], 4, 4, 2), ("group", "mp_0", "mp_1", "mp_2")
    )
    in_specs = (
        P("group", MP),
        P(None, MP),
        P(None, MP),
        P(None, MP),
        P(MP, None),
        P(MP),
        P(None, GROUP_MP, None, None),
        P("group", None),
        P("group"),
        P("group"),
        P(GROUP_MP),
        P(GROUP_MP),
    )
    out_specs = (P("group", MP), P("group"), P(None, GROUP_MP, None, None))

    return jax.shard_map(local, mesh=split, in_specs=in_specs, out_specs=out_specs, check_vma=False)
```
